32 devices in a mesh: tok: 8 (over z, y), unit: 4 (over x, core).
Axes of the slice: x: 2, y: 2, z: 4, core: 2. Of those that a mesh axis runs over, the one named last changes fastest.
Arguments:
- act_a: bfloat16 [16384, 3072], P('tok', 'unit'), may hold values from -4000 to 4000
- act_b: bfloat16 [16384, 3072], P(('tok', 'unit')), may hold values from -4000 to 4000
Outputs:
- correlation: float32 [3072, 3072], P('tok', 'unit')
The draws below stay inside these ranges and needn't reach their ends.
All inputs are finite; a program needn't handle non-finite values.
Results may differ from the reference program's by a relative error of at most 0.0003.
Values may be sent and summed in bfloat16 or wider, within the bound.
A program may use at most 128 MiB of HBM per device.

```python
import math
import jax
import jax.numpy as jnp
from jax import lax

U = 3072
TOK_DEV = 2048
TOKENS = 16384
N_TOK = 8


def shared_parts(key):
    latent = jnp.clip(jax.random.normal(jax.random.fold_in(key, 101), (TOKENS, U), jnp.float32), -6.0, 6.0)
    position = jnp.arange(TOKENS, dtype=jnp.float32) / TOKENS
    growth = math.log(3.0)
    jitter = jax.random.uniform(jax.random.fold_in(key, 102), (TOKENS,), jnp.float32, -0.6, 0.6)
    token_scale = jnp.exp(growth * position + jitter)
    return (latent, token_scale)


def own_noise(key):
    return jnp.clip(jax.random.normal(key, (TOKENS, U), jnp.float32), -6.0, 6.0)


def draw_act_a(key, part):
    latent, token_scale = shared_parts(key)
    own_key = jax.random.fold_in(key, 201)
    unit_scale = jnp.exp(jax.random.uniform(jax.random.fold_in(own_key, 1), (U,), jnp.float32, 0.0, math.log(10.0)))
    offset = jnp.clip(jax.random.normal(jax.random.fold_in(own_key, 2), (U,), jnp.float32), -3.0, 3.0)
    noise = own_noise(jax.random.fold_in(own_key, 3))
    value = unit_scale[None, :] * token_scale[:, None] * (offset[None, :] + latent + 0.7 * noise)
    return value.astype(jnp.bfloat16)


def draw_act_b(key, part):
    latent, token_scale = shared_parts(key)
    own_key = jax.random.fold_in(key, 301)
    unit_scale = jnp.exp(jax.random.uniform(jax.random.fold_in(own_key, 1), (U,), jnp.float32, 0.0, math.log(10.0)))
    offset = jnp.clip(jax.random.normal(jax.random.fold_in(own_key, 2), (U,), jnp.float32), -3.0, 3.0)
    noise = own_noise(jax.random.fold_in(own_key, 3))
    order = jax.random.permutation(jax.random.fold_in(own_key, 4), U)
    weight = jax.random.uniform(jax.random.fold_in(own_key, 5), (U,), jnp.float32, -1.2, 1.2)
    moved = jnp.take(latent, order, axis=1)
    value = unit_scale[None, :] * token_scale[:, None] * (offset[None, :] + weight[None, :] * moved + 0.7 * noise)
    return value.astype(jnp.bfloat16)


def setup_inputs(seed: int = 0) -> dict:
    keys = jax.random.split(jax.random.key(seed), 3)
    act_a = draw_act_a(jax.random.fold_in(keys[2], 71), 0)
    act_b = draw_act_b(jax.random.fold_in(keys[2], 71), 0)
    return dict(act_a=act_a, act_b=act_b)


def reference(act_a, act_b):

    def step(carry, index):
        raw, first_total, first_square, second_total, second_square = carry
        start = (index * TOK_DEV).astype(jnp.int32)
        block_a = lax.dynamic_slice_in_dim(act_a, start, TOK_DEV, 0)
        block_b = lax.dynamic_slice_in_dim(act_b, start, TOK_DEV, 0)
        raw = raw + jnp.dot(block_b.T, block_a, preferred_element_type=jnp.float32)
        wide_a = block_a.astype(jnp.float32)
        wide_b = block_b.astype(jnp.float32)
        first_total = first_total + lax.optimization_barrier(jnp.sum(wide_a, axis=0))
        first_square = first_square + lax.optimization_barrier(jnp.sum(wide_a * wide_a, axis=0))
        second_total = second_total + lax.optimization_barrier(jnp.sum(wide_b, axis=0))
        second_square = second_square + lax.optimization_barrier(jnp.sum(wide_b * wide_b, axis=0))
        return ((raw, first_total, first_square, second_total, second_square), None)
    zeros_unit = jnp.zeros((U,), jnp.float32)
    start_carry = (jnp.zeros((U, U), jnp.float32), zeros_unit, zeros_unit, zeros_unit, zeros_unit)
    final, _ = lax.scan(step, start_carry, jnp.arange(N_TOK, dtype=jnp.int32))
    raw, first_total, first_square, second_total, second_square = final
    mean_a = first_total / TOKENS
    var_a = first_square / TOKENS - mean_a * mean_a
    mean_b = second_total / TOKENS
    var_b = second_square / TOKENS - mean_b * mean_b
    centered = raw / TOKENS - mean_b[:, None] * mean_a[None, :]
    return centered / (jnp.sqrt(var_b + 1e-05)[:, None] * jnp.sqrt(var_a + 1e-05)[None, :])
```

```python
import functools

import jax
import jax.numpy as jnp
from jax import lax
from jax.experimental import pallas as pl
from jax.experimental.pallas import tpu as pltpu
from jax.sharding import PartitionSpec as P

MESH = pl.DeviceIdType.MESH
LANES = 128
SPAN = 240.0
BASE = 120.0


def contract_tokens(left, right):
    return lax.dot_general(
        left, right, (((0,), (0,)), ((), ())), preferred_element_type=jnp.float32
    )


def plain(act_a, act_b):
    token_rows = act_a.shape[0]
    units = act_b.shape[1]
    groups = lax.axis_size("tok")
    band = units // groups
    total_tokens = token_rows * groups
    wide_a = act_a.astype(jnp.float32)
    first_total = jnp.sum(wide_a, axis=0)
    first_square = jnp.sum(wide_a * wide_a, axis=0)
    piece = lax.all_gather(act_b, "unit", axis=0, tiled=True)
    product = contract_tokens(piece, act_a)
    wide_piece = piece.astype(jnp.float32)
    second_total = jnp.sum(wide_piece, axis=0)
    second_square = jnp.sum(wide_piece * wide_piece, axis=0)
    shares = lax.psum_scatter(product, "tok", scatter_dimension=0, tiled=True)
    first_all, first_square_all, second_all, second_square_all = lax.psum(
        (first_total, first_square, second_total, second_square), "tok"
    )
    offset = lax.axis_index("tok") * band
    second_own = lax.dynamic_slice_in_dim(second_all, offset, band, 0)
    second_square_own = lax.dynamic_slice_in_dim(second_square_all, offset, band, 0)
    mean_a = first_all / total_tokens
    var_a = first_square_all / total_tokens - mean_a * mean_a
    mean_b = second_own / total_tokens
    var_b = second_square_own / total_tokens - mean_b * mean_b
    centered = shares / total_tokens - mean_b[:, None] * mean_a[None, :]
    return centered / (jnp.sqrt(var_b + 1e-05)[:, None] * jnp.sqrt(var_a + 1e-05)[None, :])


def schedule(rings, parts):
    crosses, keeps = rings * parts, (rings - 1) * parts
    events = sorted(
        [(k / crosses, 0, k) for k in range(crosses)] + [((k + 0.2) / keeps, 1, k) for k in range(keeps)]
    )
    slots = [(kind, k) for _, kind, k in events] + [(1, keeps + i) for i in range(parts)]
    place = {slot: s for s, slot in enumerate(slots)}
    orders = []
    for r in range(rings):
        behind = lambda d: r if d > r else rings - 1 - r
        others = [d for d in range(rings) if d != r]
        orders.append(sorted(others, key=lambda d: (-abs(d - r), -behind(d), d)) + [r])
    done = [{} for _ in range(rings)]
    merges = [[0] * len(slots) for _ in range(rings)]
    for s in range(crosses + keeps):
        for r in range(rings):
            k = len(done[r])
            if k == keeps or place[1, k] + 1 > s or place[0, k] + 3 > s:
                continue
            d, i = orders[r][k // parts], k % parts
            before = r - 1 if d > r else r + 1
            if 0 <= before < rings and done[before].get((d, i), s) + 3 > s:
                continue
            done[r][d, i] = s
            merges[r][s] = k + 1
    complete = all(len(d) == keeps for d in done)
    return slots, orders, merges, complete


def pick(values, i):
    out = values[-1]
    for k in reversed(range(len(values) - 1)):
        if values[k] != values[k + 1] or not isinstance(out, (int, float)):
            out = jnp.where(i == k, values[k], out)
    return out


def pick_row(rows, r, i):
    out = None
    unique = []
    for row in rows:
        if row not in unique:
            unique.append(row)
    for row in unique:
        mine = pick(row, i)
        if out is None:
            out = mine
        else:
            here = functools.reduce(jnp.logical_or, [r == k for k in range(len(rows)) if rows[k] == row])
            out = jnp.where(here, mine, out)
    return out


def column(row):
    return jnp.transpose(jnp.broadcast_to(row, (LANES, LANES)))


def spread(square, total, share):
    return jnp.maximum(square - total * total * share, square * 1e-5 + 1e-30)


def encode(q):
    size = jnp.exp2(jnp.minimum(jnp.abs(q), 1.04) * SPAN - BASE)
    return jnp.where(q < 0, -size, size).astype(jnp.bfloat16)


def decode(code):
    y = code.astype(jnp.float32)
    size = jnp.log2(jnp.abs(y)) + BASE
    return jnp.where(y < 0, -size, size)


def kernel(groups, plan, a_hbm, b_hbm, out, a, g, held, cross_out, cross_in, far_out, far_in,
           sa_own, sa_near, sa_pair, sa_in, sa_run, sa_stat, sb_half, sb_mine, sb_near, sb_run, sb_in,
           a_sem, b_sem, px_send, px_recv, nx_send, nx_recv, fw_send, fw_recv,
           c_send, c_recv, cb_send, cb_recv, f_send, f_recv, fb_send, fb_recv,
           ca_send, ca_recv, fa_send, fa_recv):
    slots, orders, merges, _ = plan
    t = lax.axis_index("tok")
    u = lax.axis_index("unit")
    rows, units = b_hbm.shape
    tokens, own = a.shape
    band = units // groups
    parts = band // LANES
    rings = groups // 2
    crosses = rings * parts
    keeps = crosses - parts
    steps = len(slots)
    half = tokens // 2
    r = t // 2
    y = t % 2
    side = u // 2
    partner = u + 1 - 2 * (u % 2)
    across = (u + 2) % 4
    near = t + 1 - 2 * y
    shares = [1.0 / (2 * tokens * max(k, 1)) for k in range(rings + 1)]
    packed = [kind + 2 * (k // parts) + 2048 * (k % parts) for kind, k in slots]

    def slot(s):
        code = pick(packed, s)
        kind, p, i = code % 2, (code // 2) % 1024, code // 2048
        return kind, p, i

    def bound(p):
        return pick_row(orders, r, p)

    def columns(kind, p, i):
        owner = bound(p) * 2 + jnp.where(kind == 0, 1 - y, y)
        return pl.ds(pl.multiple_of(owner * band + i * LANES, LANES), LANES)

    def block(ref, who, cols):
        return ref.at[pl.ds(pl.multiple_of(who * rows, rows), rows), cols]

    def remote(src, dst, send, recv, tt, uu):
        return pltpu.make_async_remote_copy(
            src_ref=src, dst_ref=dst, send_sem=send, recv_sem=recv,
            device_id=(tt, uu), device_id_type=MESH)

    def to_partner(s, cols):
        return remote(b_hbm.at[:, cols], block(g, u, cols), px_send.at[s], px_recv.at[s], t, partner)

    def to_across(s, cols):
        return remote(b_hbm.at[:, cols], block(g, u, cols), nx_send.at[s], nx_recv.at[s], t, across)

    def forward(s, cols):
        return remote(block(g, across, cols), block(g, across, cols), fw_send.at[s], fw_recv.at[s],
                      t, partner)

    def send_cross(k):
        return remote(cross_out.at[k], cross_in.at[k], c_send.at[k], c_recv.at[k], near, u)

    def send_cross_sums(k):
        return remote(sb_mine.at[k], sb_near.at[k], cb_send.at[k], cb_recv.at[k], near, u)

    def send_far(k, j, tt):
        return remote(far_out.at[k], far_in.at[j], f_send.at[k], f_recv.at[j], tt, u)

    def send_far_sums(k, j, tt):
        return remote(sb_run.at[k], sb_in.at[j], fb_send.at[k], fb_recv.at[j], tt, u)

    send_near_a = remote(sa_own, sa_near, ca_send.at[0], ca_recv.at[0], near, u)

    def send_run_a(way):
        tt = t + 2 if way == 0 else t - 2
        return remote(sa_run.at[way], sa_in.at[way], fa_send.at[way], fa_recv.at[way], tt, u)

    a_copy = pltpu.make_async_copy(a_hbm, a, a_sem)
    own_rows = pl.ds(pl.multiple_of(u * rows, rows), rows)
    b_copy = pltpu.make_async_copy(b_hbm, g.at[own_rows, :], b_sem)

    barrier = pltpu.get_barrier_semaphore()

    def greet(tt, uu):
        pl.semaphore_signal(barrier, inc=1, device_id=(tt, uu), device_id_type=MESH)

    greet(t, across)
    greet(t, partner)
    greet(near, u)

    @pl.when(r > 0)
    def _():
        greet(t - 2, u)

    @pl.when(r < rings - 1)
    def _():
        greet(t + 2, u)

    a_copy.start()
    b_copy.start()
    pl.semaphore_wait(barrier, 3 + jnp.where(r > 0, 1, 0) + jnp.where(r < rings - 1, 1, 0))

    @pl.loop(0, steps)
    def _(s):
        cols = columns(*slot(s))
        to_across(s, cols).start()
        to_partner(s, cols).start()

    a_copy.wait()
    b_copy.wait()
    chunk = 128

    def sum_rows(wide):
        wide = wide.astype(jnp.float32).reshape(wide.shape[0] // 8, 8, wide.shape[1])
        return jnp.sum(wide, axis=0), jnp.sum(wide * wide, axis=0)

    def body(i, carry):
        total, square = sum_rows(a[pl.ds(pl.multiple_of(i * chunk, chunk), chunk), :])
        return carry[0] + total, carry[1] + square

    zero = jnp.zeros((8, own), jnp.float32)
    total, square = lax.fori_loop(0, tokens // chunk, body, (zero, zero))
    sa_own[...] = jnp.zeros((8, own), jnp.float32)
    sa_own[0:1, :] = jnp.sum(total, axis=0, keepdims=True)
    sa_own[1:2, :] = jnp.sum(square, axis=0, keepdims=True)
    send_near_a.start()

    def tiles():
        return [slice(c * LANES, (c + 1) * LANES) for c in range(own // LANES)]

    def early(hold, cols):
        mine = pl.ds(pl.multiple_of(side * half, half), half)
        lhs = g[mine, cols]
        held[hold] = contract_tokens(lhs, a[mine, :])
        total, square = sum_rows(lhs)
        sb_half[0] = total
        sb_half[1] = square

    def late(hold, slot_sums, cols):
        theirs = pl.ds(pl.multiple_of((1 - side) * half, half), half)
        lhs = g[theirs, cols]
        held[hold] = held[hold] + contract_tokens(lhs, a[theirs, :])
        total, square = sum_rows(lhs)
        sb_mine[slot_sums] = jnp.zeros((8, LANES), jnp.float32)
        sb_mine[slot_sums, 0:1, :] = jnp.sum(sb_half[0] + total, axis=0, keepdims=True)
        sb_mine[slot_sums, 1:2, :] = jnp.sum(sb_half[1] + square, axis=0, keepdims=True)

    def put(target, k, hold, sb, sa, share):
        tb, qb = sb[0:1, :], sb[1:2, :]
        tb_col = column(tb * share)
        scale_col = column(lax.rsqrt(spread(qb, tb, share)))
        for cols in tiles():
            ta = sa[0:1, cols]
            scale = lax.rsqrt(spread(sa[1:2, cols], ta, share))
            q = (held[hold, :, cols] - tb_col * ta) * (scale_col * scale)
            target[k, :, cols] = encode(q)

    def take(hold, source, k, sb, sa, share):
        tb, qb = sb[0:1, :], sb[1:2, :]
        tb_col = column(tb * share)
        norm_col = column(jnp.sqrt(spread(qb, tb, share)) * (1.0 / SPAN))
        for cols in tiles():
            ta = sa[0:1, cols]
            norm = jnp.sqrt(spread(sa[1:2, cols], ta, share))
            held[hold, :, cols] = held[hold, :, cols] + (
                decode(source[k, :, cols]) * (norm_col * norm) + tb_col * ta)

    def take_near(k):
        send_cross_sums(k).wait_recv()
        send_cross(k).wait_recv()
        take(k, cross_in, k, sb_near.at[k], sa_near, 1.0 / tokens)

    def take_far(way, k, j):
        tt = t + 2 - 4 * way
        send_far_sums(0, j, tt).wait_recv()
        send_far(0, j, tt).wait_recv()
        count = jnp.where(way == 0, r, rings - 1 - r)
        take(k, far_in, j, sb_in.at[j], sa_in.at[way], pick(shares, count))

    def merge(k):
        p, i = k // parts, k % parts
        d = bound(p)
        way = jnp.where(d > r, 0, 1)
        j = (way * rings + d) * parts + i
        take_near(k)
        sb_run[k] = sb_mine[crosses + k] + sb_near[k]
        count = jnp.where(way == 0, r, rings - 1 - r)

        @pl.when(count > 0)
        def _():
            take_far(way, k, j)
            sb_run[k] = sb_run[k] + sb_in[j]

        put(far_out, k, k, sb_run.at[k], sa_run.at[way], pick(shares, count + 1))
        tt = t + 2 - 4 * way
        send_far(k, j, tt).start()
        send_far_sums(k, j, tt).start()

    def exchange_a(s):
        @pl.when(s == 1)
        def _():
            send_near_a.wait_recv()
            sa_pair[...] = sa_own[...] + sa_near[...]

        for way, ready in ((0, r + 1), (1, rings - r)):
            first = (r == 0) if way == 0 else (r == rings - 1)
            final = (r == rings - 1) if way == 0 else (r == 0)

            @pl.when(jnp.logical_and(s == ready, first))
            def _():
                sa_in[way] = jnp.zeros((8, own), jnp.float32)
                sa_run[way] = sa_pair[...]

            @pl.when(jnp.logical_and(s == ready, jnp.logical_not(first)))
            def _():
                send_run_a(way).wait_recv()
                sa_run[way] = sa_pair[...] + sa_in[way]

            @pl.when(jnp.logical_and(s == ready, jnp.logical_not(final)))
            def _():
                send_run_a(way).start()

    @pl.loop(0, steps - parts)
    def _(s):
        kind, p, i = slot(s)
        cols = columns(kind, p, i)
        k = p * parts + i
        hold = jnp.where(kind == 0, crosses, k)
        to_partner(s, cols).wait_recv()
        early(hold, cols)
        to_across(s, cols).wait_recv()
        forward(s, cols).start()
        exchange_a(s)
        pair = pick_row(merges, r, s)

        @pl.when(pair > 0)
        def _():
            merge(pair - 1)

        forward(s, cols).wait_recv()
        late(hold, kind * crosses + k, cols)

        @pl.when(kind == 0)
        def _():
            put(cross_out, k, hold, sb_mine.at[k], sa_own, 1.0 / tokens)
            send_cross(k).start()
            send_cross_sums(k).start()

    whole_a = sa_pair[...] + sa_in[0] + sa_in[1]
    total_tokens = tokens * groups
    mean_a = whole_a[0:1, :] * (1.0 / total_tokens)
    var_a = whole_a[1:2, :] * (1.0 / total_tokens) - mean_a * mean_a
    sa_stat[0:1, :] = mean_a
    sa_stat[1:2, :] = 1.0 / jnp.sqrt(var_a + 1e-05)

    @pl.loop(0, parts)
    def _(i):
        s = steps - parts + i
        k = keeps + i
        cols = pl.ds(pl.multiple_of(t * band + i * LANES, LANES), LANES)
        to_partner(s, cols).wait_recv()
        early(k, cols)
        to_across(s, cols).wait_recv()
        forward(s, cols).start()
        take_near(k)
        sb_half[2] = sb_near[k]
        for way, some in ((0, r > 0), (1, r < rings - 1)):
            @pl.when(some)
            def _():
                j = (way * rings + r) * parts + i
                take_far(way, k, j)
                sb_half[2] = sb_half[2] + sb_in[j]

        forward(s, cols).wait_recv()
        late(k, crosses + k, cols)
        whole_b = sb_half[2] + sb_mine[crosses + k]
        mean_b = whole_b[0:1, :] * (1.0 / total_tokens)
        var_b = whole_b[1:2, :] * (1.0 / total_tokens) - mean_b * mean_b
        mean_col = column(mean_b)
        inv_col = column(1.0 / jnp.sqrt(var_b + 1e-05))
        lanes = pl.ds(pl.multiple_of(i * LANES, LANES), LANES)
        for c in tiles():
            centered = held[k, :, c] * (1.0 / total_tokens) - mean_col * sa_stat[0:1, c]
            out[lanes, c] = centered * (inv_col * sa_stat[1:2, c])

    send_near_a.wait_send()

    @pl.when(r < rings - 1)
    def _():
        send_run_a(0).wait_send()

    @pl.when(r > 0)
    def _():
        send_run_a(1).wait_send()

    @pl.loop(0, keeps)
    def _(k):
        send_far(k, 0, near).wait_send()
        send_far_sums(k, 0, near).wait_send()

    @pl.loop(0, crosses)
    def _(k):
        send_cross(k).wait_send()
        send_cross_sums(k).wait_send()

    @pl.loop(0, steps)
    def _(s):
        cols = pl.ds(0, LANES)
        to_across(s, cols).wait_send()
        to_partner(s, cols).wait_send()
        forward(s, cols).wait_send()


def fused(groups, plan, act_a, act_b):
    tokens, own = act_a.shape
    rows, units = act_b.shape
    band = units // groups
    parts = band // LANES
    rings = groups // 2
    crosses = rings * parts
    keeps = crosses - parts
    steps = 2 * crosses
    dma = lambda n: pltpu.SemaphoreType.DMA((n,))
    bf16 = lambda *shape: pltpu.VMEM(shape, jnp.bfloat16)
    f32 = lambda *shape: pltpu.VMEM(shape, jnp.float32)
    return pl.pallas_call(
        functools.partial(kernel, groups, plan),
        out_shape=jax.ShapeDtypeStruct((band, own), jnp.float32),
        in_specs=[pl.BlockSpec(memory_space=pltpu.HBM)] * 2,
        out_specs=pl.BlockSpec(memory_space=pltpu.VMEM),
        scratch_shapes=[
            bf16(tokens, own),
            bf16(tokens, units),
            f32(crosses + 1, LANES, own),
            bf16(crosses, LANES, own),
            bf16(crosses, LANES, own),
            bf16(keeps, LANES, own),
            bf16(2 * crosses, LANES, own),
            f32(8, own), f32(8, own), f32(8, own),
            f32(2, 8, own), f32(2, 8, own), f32(8, own),
            f32(3, 8, LANES),
            f32(2 * crosses, 8, LANES), f32(crosses, 8, LANES),
            f32(keeps, 8, LANES), f32(2 * crosses, 8, LANES),
            pltpu.SemaphoreType.DMA, pltpu.SemaphoreType.DMA,
            dma(steps), dma(steps),
            dma(steps), dma(steps),
            dma(steps), dma(steps),
            dma(crosses), dma(crosses),
            dma(crosses), dma(crosses),
            dma(keeps), dma(2 * crosses),
            dma(keeps), dma(2 * crosses),
            dma(1), dma(1),
            dma(2), dma(2),
        ],
        compiler_params=pltpu.CompilerParams(
            collective_id=0, has_side_effects=True, vmem_limit_bytes=60000 * 1024
        ),
        name="gather_correlate",
    )(act_a, act_b)


def solution(mesh):
    groups, split = mesh.shape["tok"], mesh.shape["unit"]

    def per_device(act_a, act_b):
        band = act_b.shape[1] // groups
        whole = act_a.shape[0] % 256 == 0 and act_a.shape[1] % LANES == 0
        if split == 4 and groups % 2 == 0 and groups > 4 and band % LANES == 0 and whole:
            plan = schedule(groups // 2, band // LANES)
            if plan[-1]:
                return fused(groups, plan, act_a, act_b)
        return plain(act_a, act_b)

    placed = (P("tok", "unit"), P(("tok", "unit"), None))
    return jax.shard_map(
        per_device, mesh=mesh, in_specs=placed, out_specs=P("tok", "unit"), check_vma=False
    )
```

```python
import functools

import jax
import jax.numpy as jnp
from jax import lax
from jax.experimental import pallas as pl
from jax.experimental.pallas import tpu as pltpu
from jax.sharding import PartitionSpec as P

MESH = pl.DeviceIdType.MESH
LANES = 128
SPAN = 240.0
BASE = 120.0


def contract_tokens(left, right):
    return lax.dot_general(
        left, right, (((0,), (0,)), ((), ())), preferred_element_type=jnp.float32
    )


def plain(act_a, act_b):
    token_rows = act_a.shape[0]
    units = act_b.shape[1]
    groups = lax.axis_size("tok")
    band = units // groups
    total_tokens = token_rows * groups
    wide_a = act_a.astype(jnp.float32)
    first_total = jnp.sum(wide_a, axis=0)
    first_square = jnp.sum(wide_a * wide_a, axis=0)
    piece = lax.all_gather(act_b, "unit", axis=0, tiled=True)
    product = contract_tokens(piece, act_a)
    wide_piece = piece.astype(jnp.float32)
    second_total = jnp.sum(wide_piece, axis=0)
    second_square = jnp.sum(wide_piece * wide_piece, axis=0)
    shares = lax.psum_scatter(product, "tok", scatter_dimension=0, tiled=True)
    first_all, first_square_all, second_all, second_square_all = lax.psum(
        (first_total, first_square, second_total, second_square), "tok"
    )
    offset = lax.axis_index("tok") * band
    second_own = lax.dynamic_slice_in_dim(second_all, offset, band, 0)
    second_square_own = lax.dynamic_slice_in_dim(second_square_all, offset, band, 0)
    mean_a = first_all / total_tokens
    var_a = first_square_all / total_tokens - mean_a * mean_a
    mean_b = second_own / total_tokens
    var_b = second_square_own / total_tokens - mean_b * mean_b
    centered = shares / total_tokens - mean_b[:, None] * mean_a[None, :]
    return centered / (jnp.sqrt(var_b + 1e-05)[:, None] * jnp.sqrt(var_a + 1e-05)[None, :])


def schedule(rings, parts):
    crosses, keeps = rings * parts, (rings - 1) * parts
    events = sorted(
        [((k + 0.25) / crosses, 0, k) for k in range(crosses)]
        + [((k + 1) / keeps, 1, k) for k in range(keeps)]
    )
    slots = [(kind, k) for _, kind, k in events] + [(1, keeps + i) for i in range(parts)]
    place = {slot: s for s, slot in enumerate(slots)}
    orders = []
    for r in range(rings):
        behind = lambda d: r if d > r else rings - 1 - r
        others = [d for d in range(rings) if d != r]
        orders.append(sorted(others, key=lambda d: (-abs(d - r), -behind(d), d)) + [r])
    done = [{} for _ in range(rings)]
    merges = [[0] * len(slots) for _ in range(rings)]
    for s in range(crosses + keeps):
        for r in range(rings):
            k = len(done[r])
            if k == keeps or place[1, k] > s or place[0, k] + 3 > s:
                continue
            d, i = orders[r][k // parts], k % parts
            before = r - 1 if d > r else r + 1
            if 0 <= before < rings and done[before].get((d, i), s) + 3 > s:
                continue
            done[r][d, i] = s
            merges[r][s] = k + 1
    complete = all(len(d) == keeps for d in done)
    return slots, orders, merges, complete


def pick(values, i):
    out = values[-1]
    for k in reversed(range(len(values) - 1)):
        if values[k] != values[k + 1] or not isinstance(out, (int, float)):
            out = jnp.where(i == k, values[k], out)
    return out


def pick_row(rows, r, i):
    out = None
    unique = []
    for row in rows:
        if row not in unique:
            unique.append(row)
    for row in unique:
        mine = pick(row, i)
        if out is None:
            out = mine
        else:
            here = functools.reduce(jnp.logical_or, [r == k for k in range(len(rows)) if rows[k] == row])
            out = jnp.where(here, mine, out)
    return out


def column(row):
    return jnp.transpose(jnp.broadcast_to(row, (LANES, LANES)))


def spread(square, total, share):
    return jnp.maximum(square - total * total * share, square * 1e-5 + 1e-30)


def encode(q):
    size = jnp.exp2(jnp.minimum(jnp.abs(q), 1.04) * SPAN - BASE)
    return jnp.where(q < 0, -size, size).astype(jnp.bfloat16)


def decode(code):
    y = code.astype(jnp.float32)
    size = jnp.log2(jnp.abs(y)) + BASE
    return jnp.where(y < 0, -size, size)


def kernel(groups, plan, a_hbm, b_hbm, out, a, g, held, cross_out, cross_in, far_out, far_in,
           sa_own, sa_near, sa_pair, sa_in, sa_run, sa_stat, sb_half, sb_mine, sb_near, sb_run, sb_in,
           a_sem, b_sem, px_send, px_recv, nx_send, nx_recv, fw_send, fw_recv,
           c_send, c_recv, cb_send, cb_recv, f_send, f_recv, fb_send, fb_recv,
           ca_send, ca_recv, fa_send, fa_recv):
    slots, orders, merges, _ = plan
    t = lax.axis_index("tok")
    u = lax.axis_index("unit")
    rows, units = b_hbm.shape
    tokens, own = a.shape
    band = units // groups
    parts = band // LANES
    rings = groups // 2
    crosses = rings * parts
    keeps = crosses - parts
    steps = len(slots)
    half = tokens // 2
    r = t // 2
    y = t % 2
    side = u // 2
    partner = u + 1 - 2 * (u % 2)
    across = (u + 2) % 4
    near = t + 1 - 2 * y
    shares = [1.0 / (2 * tokens * max(k, 1)) for k in range(rings + 1)]
    packed = [kind + 2 * (k // parts) + 2048 * (k % parts) for kind, k in slots]

    def slot(s):
        code = pick(packed, s)
        kind, p, i = code % 2, (code // 2) % 1024, code // 2048
        return kind, p, i

    def bound(p):
        return pick_row(orders, r, p)

    def columns(kind, p, i):
        owner = bound(p) * 2 + jnp.where(kind == 0, 1 - y, y)
        return pl.ds(pl.multiple_of(owner * band + i * LANES, LANES), LANES)

    def block(ref, who, cols):
        return ref.at[pl.ds(pl.multiple_of(who * rows, rows), rows), cols]

    def remote(src, dst, send, recv, tt, uu):
        return pltpu.make_async_remote_copy(
            src_ref=src, dst_ref=dst, send_sem=send, recv_sem=recv,
            device_id=(tt, uu), device_id_type=MESH)

    def to_partner(s, cols):
        return remote(b_hbm.at[:, cols], block(g, u, cols), px_send.at[0], px_recv.at[s], t, partner)

    def to_across(s, cols):
        return remote(b_hbm.at[:, cols], block(g, u, cols), nx_send.at[0], nx_recv.at[s], t, across)

    def forward(s, cols):
        return remote(block(g, across, cols), block(g, across, cols), fw_send.at[0], fw_recv.at[s],
                      t, partner)

    def send_cross(k):
        return remote(cross_out.at[k], cross_in.at[k], c_send.at[0], c_recv.at[k], near, u)

    def send_cross_sums(k):
        return remote(sb_mine.at[k], sb_near.at[k], cb_send.at[0], cb_recv.at[k], near, u)

    def send_far(k, j, tt):
        return remote(far_out.at[k], far_in.at[j], f_send.at[0], f_recv.at[j], tt, u)

    def send_far_sums(k, j, tt):
        return remote(sb_run.at[k], sb_in.at[j], fb_send.at[0], fb_recv.at[j], tt, u)

    send_near_a = remote(sa_own, sa_near, ca_send.at[0], ca_recv.at[0], near, u)

    def send_run_a(way):
        tt = t + 2 if way == 0 else t - 2
        return remote(sa_run.at[way], sa_in.at[way], fa_send.at[way], fa_recv.at[way], tt, u)

    a_copy = pltpu.make_async_copy(a_hbm, a, a_sem)
    own_rows = pl.ds(pl.multiple_of(u * rows, rows), rows)
    b_copy = pltpu.make_async_copy(b_hbm, g.at[own_rows, :], b_sem)

    barrier = pltpu.get_barrier_semaphore()

    def greet(tt, uu):
        pl.semaphore_signal(barrier, inc=1, device_id=(tt, uu), device_id_type=MESH)

    greet(t, across)
    greet(t, partner)
    greet(near, u)

    @pl.when(r > 0)
    def _():
        greet(t - 2, u)

    @pl.when(r < rings - 1)
    def _():
        greet(t + 2, u)

    a_copy.start()
    b_copy.start()
    pl.semaphore_wait(barrier, 3 + jnp.where(r > 0, 1, 0) + jnp.where(r < rings - 1, 1, 0))

    @pl.loop(0, steps)
    def _(s):
        cols = columns(*slot(s))
        to_across(s, cols).start()
        to_partner(s, cols).start()

    a_copy.wait()
    b_copy.wait()
    chunk = 128

    def sum_rows(wide):
        wide = wide.astype(jnp.float32).reshape(wide.shape[0] // 8, 8, wide.shape[1])
        return jnp.sum(wide, axis=0), jnp.sum(wide * wide, axis=0)

    def body(i, carry):
        total, square = sum_rows(a[pl.ds(pl.multiple_of(i * chunk, chunk), chunk), :])
        return carry[0] + total, carry[1] + square

    zero = jnp.zeros((8, own), jnp.float32)
    total, square = lax.fori_loop(0, tokens // chunk, body, (zero, zero))
    sa_own[...] = jnp.zeros((8, own), jnp.float32)
    sa_own[0:1, :] = jnp.sum(total, axis=0, keepdims=True)
    sa_own[1:2, :] = jnp.sum(square, axis=0, keepdims=True)
    send_near_a.start()

    def tiles():
        return [slice(c * LANES, (c + 1) * LANES) for c in range(own // LANES)]

    def early(hold, cols):
        mine = pl.ds(pl.multiple_of(side * half, half), half)
        lhs = g[mine, cols]
        held[hold] = contract_tokens(lhs, a[mine, :])
        total, square = sum_rows(lhs)
        sb_half[0] = total
        sb_half[1] = square

    def late(hold, slot_sums, cols):
        theirs = pl.ds(pl.multiple_of((1 - side) * half, half), half)
        lhs = g[theirs, cols]
        held[hold] = held[hold] + contract_tokens(lhs, a[theirs, :])
        total, square = sum_rows(lhs)
        sb_mine[slot_sums] = jnp.zeros((8, LANES), jnp.float32)
        sb_mine[slot_sums, 0:1, :] = jnp.sum(sb_half[0] + total, axis=0, keepdims=True)
        sb_mine[slot_sums, 1:2, :] = jnp.sum(sb_half[1] + square, axis=0, keepdims=True)

    def put(target, k, hold, sb, sa, share):
        tb, qb = sb[0:1, :], sb[1:2, :]
        tb_col = column(tb * share)
        scale_col = column(lax.rsqrt(spread(qb, tb, share)))
        for cols in tiles():
            ta = sa[0:1, cols]
            scale = lax.rsqrt(spread(sa[1:2, cols], ta, share))
            q = (held[hold, :, cols] - tb_col * ta) * (scale_col * scale)
            target[k, :, cols] = encode(q)

    def take(hold, source, k, sb, sa, share):
        tb, qb = sb[0:1, :], sb[1:2, :]
        tb_col = column(tb * share)
        norm_col = column(jnp.sqrt(spread(qb, tb, share)) * (1.0 / SPAN))
        for cols in tiles():
            ta = sa[0:1, cols]
            norm = jnp.sqrt(spread(sa[1:2, cols], ta, share))
            held[hold, :, cols] = held[hold, :, cols] + (
                decode(source[k, :, cols]) * (norm_col * norm) + tb_col * ta)

    def take_near(k):
        send_cross_sums(k).wait_recv()
        send_cross(k).wait_recv()
        take(k, cross_in, k, sb_near.at[k], sa_near, 1.0 / tokens)

    def take_far(way, k, j):
        tt = t + 2 - 4 * way
        send_far_sums(0, j, tt).wait_recv()
        send_far(0, j, tt).wait_recv()
        count = jnp.where(way == 0, r, rings - 1 - r)
        take(k, far_in, j, sb_in.at[j], sa_in.at[way], pick(shares, count))

    def merge(k):
        p, i = k // parts, k % parts
        d = bound(p)
        way = jnp.where(d > r, 0, 1)
        j = (way * rings + d) * parts + i
        take_near(k)
        sb_run[k] = sb_mine[crosses + k] + sb_near[k]
        count = jnp.where(way == 0, r, rings - 1 - r)

        @pl.when(count > 0)
        def _():
            take_far(way, k, j)
            sb_run[k] = sb_run[k] + sb_in[j]

        put(far_out, k, k, sb_run.at[k], sa_run.at[way], pick(shares, count + 1))
        tt = t + 2 - 4 * way
        send_far(k, j, tt).start()
        send_far_sums(k, j, tt).start()

    def exchange_a(s):
        @pl.when(s == 1)
        def _():
            send_near_a.wait_recv()
            sa_pair[...] = sa_own[...] + sa_near[...]

        for way, ready in ((0, r + 1), (1, rings - r)):
            first = (r == 0) if way == 0 else (r == rings - 1)
            final = (r == rings - 1) if way == 0 else (r == 0)

            @pl.when(jnp.logical_and(s == ready, first))
            def _():
                sa_in[way] = jnp.zeros((8, own), jnp.float32)
                sa_run[way] = sa_pair[...]

            @pl.when(jnp.logical_and(s == ready, jnp.logical_not(first)))
            def _():
                send_run_a(way).wait_recv()
                sa_run[way] = sa_pair[...] + sa_in[way]

            @pl.when(jnp.logical_and(s == ready, jnp.logical_not(final)))
            def _():
                send_run_a(way).start()

    @pl.loop(0, steps - parts)
    def _(s):
        kind, p, i = slot(s)
        cols = columns(kind, p, i)
        k = p * parts + i
        hold = jnp.where(kind == 0, crosses, k)
        to_partner(s, cols).wait_recv()
        early(hold, cols)
        to_across(s, cols).wait_recv()
        forward(s, cols).start()
        exchange_a(s)
        forward(s, cols).wait_recv()
        late(hold, kind * crosses + k, cols)

        @pl.when(kind == 0)
        def _():
            put(cross_out, k, hold, sb_mine.at[k], sa_own, 1.0 / tokens)
            send_cross(k).start()
            send_cross_sums(k).start()

        pair = pick_row(merges, r, s)

        @pl.when(pair > 0)
        def _():
            merge(pair - 1)

    whole_a = sa_pair[...] + sa_in[0] + sa_in[1]
    total_tokens = tokens * groups
    mean_a = whole_a[0:1, :] * (1.0 / total_tokens)
    var_a = whole_a[1:2, :] * (1.0 / total_tokens) - mean_a * mean_a
    sa_stat[0:1, :] = mean_a
    sa_stat[1:2, :] = 1.0 / jnp.sqrt(var_a + 1e-05)

    @pl.loop(0, parts)
    def _(i):
        s = steps - parts + i
        k = keeps + i
        cols = pl.ds(pl.multiple_of(t * band + i * LANES, LANES), LANES)
        to_partner(s, cols).wait_recv()
        early(k, cols)
        to_across(s, cols).wait_recv()
        forward(s, cols).start()
        take_near(k)
        sb_half[2] = sb_near[k]
        for way, some in ((0, r > 0), (1, r < rings - 1)):
            @pl.when(some)
            def _():
                j = (way * rings + r) * parts + i
                take_far(way, k, j)
                sb_half[2] = sb_half[2] + sb_in[j]

        forward(s, cols).wait_recv()
        late(k, crosses + k, cols)
        whole_b = sb_half[2] + sb_mine[crosses + k]
        mean_b = whole_b[0:1, :] * (1.0 / total_tokens)
        var_b = whole_b[1:2, :] * (1.0 / total_tokens) - mean_b * mean_b
        mean_col = column(mean_b)
        inv_col = column(1.0 / jnp.sqrt(var_b + 1e-05))
        lanes = pl.ds(pl.multiple_of(i * LANES, LANES), LANES)
        for c in tiles():
            centered = held[k, :, c] * (1.0 / total_tokens) - mean_col * sa_stat[0:1, c]
            out[lanes, c] = centered * (inv_col * sa_stat[1:2, c])

    send_near_a.wait_send()

    @pl.when(r < rings - 1)
    def _():
        send_run_a(0).wait_send()

    @pl.when(r > 0)
    def _():
        send_run_a(1).wait_send()

    own_b = g.at[own_rows, :]
    remote(b_hbm, own_b, nx_send.at[0], nx_recv.at[0], t, across).wait_send()
    remote(b_hbm, own_b, px_send.at[0], px_recv.at[0], t, partner).wait_send()
    remote(own_b, own_b, fw_send.at[0], fw_recv.at[0], t, partner).wait_send()
    remote(cross_out, cross_in, c_send.at[0], c_recv.at[0], near, u).wait_send()
    remote(sb_near, sb_near, cb_send.at[0], cb_recv.at[0], near, u).wait_send()
    remote(far_out, far_out, f_send.at[0], f_recv.at[0], near, u).wait_send()
    remote(sb_run, sb_run, fb_send.at[0], fb_recv.at[0], near, u).wait_send()


def fused(groups, plan, act_a, act_b):
    tokens, own = act_a.shape
    rows, units = act_b.shape
    band = units // groups
    parts = band // LANES
    rings = groups // 2
    crosses = rings * parts
    keeps = crosses - parts
    steps = 2 * crosses
    dma = lambda n: pltpu.SemaphoreType.DMA((n,))
    bf16 = lambda *shape: pltpu.VMEM(shape, jnp.bfloat16)
    f32 = lambda *shape: pltpu.VMEM(shape, jnp.float32)
    return pl.pallas_call(
        functools.partial(kernel, groups, plan),
        out_shape=jax.ShapeDtypeStruct((band, own), jnp.float32),
        in_specs=[pl.BlockSpec(memory_space=pltpu.HBM)] * 2,
        out_specs=pl.BlockSpec(memory_space=pltpu.VMEM),
        scratch_shapes=[
            bf16(tokens, own),
            bf16(tokens, units),
            f32(crosses + 1, LANES, own),
            bf16(crosses, LANES, own),
            bf16(crosses, LANES, own),
            bf16(keeps, LANES, own),
            bf16(2 * crosses, LANES, own),
            f32(8, own), f32(8, own), f32(8, own),
            f32(2, 8, own), f32(2, 8, own), f32(8, own),
            f32(3, 8, LANES),
            f32(2 * crosses, 8, LANES), f32(crosses, 8, LANES),
            f32(keeps, 8, LANES), f32(2 * crosses, 8, LANES),
            pltpu.SemaphoreType.DMA, pltpu.SemaphoreType.DMA,
            dma(1), dma(steps),
            dma(1), dma(steps),
            dma(1), dma(steps),
            dma(1), dma(crosses),
            dma(1), dma(crosses),
            dma(1), dma(2 * crosses),
            dma(1), dma(2 * crosses),
            dma(1), dma(1),
            dma(2), dma(2),
        ],
        compiler_params=pltpu.CompilerParams(
            collective_id=0, has_side_effects=True, vmem_limit_bytes=52000 * 1024
        ),
        name="gather_correlate",
    )(act_a, act_b)


def solution(mesh):
    groups, split = mesh.shape["tok"], mesh.shape["unit"]

    def per_device(act_a, act_b):
        band = act_b.shape[1] // groups
        whole = act_a.shape[0] % 256 == 0 and act_a.shape[1] % LANES == 0
        if split == 4 and groups % 2 == 0 and groups > 4 and band % LANES == 0 and whole:
            plan = schedule(groups // 2, band // LANES)
            if plan[-1]:
                return fused(groups, plan, act_a, act_b)
        return plain(act_a, act_b)

    placed = (P("tok", "unit"), P(("tok", "unit"), None))
    return jax.shard_map(
        per_device, mesh=mesh, in_specs=placed, out_specs=P("tok", "unit"), check_vma=False
    )
```

```python
import functools

import jax
import jax.numpy as jnp
from jax import lax
from jax.experimental import pallas as pl
from jax.experimental.pallas import tpu as pltpu
from jax.sharding import PartitionSpec as P

MESH = pl.DeviceIdType.MESH
LANES = 128
SPAN = 240.0
BASE = 120.0
AHEAD = 4
BUNCHES = 4


def contract_tokens(left, right):
    return lax.dot_general(
        left, right, (((0,), (0,)), ((), ())), preferred_element_type=jnp.float32
    )


def plain(act_a, act_b):
    token_rows = act_a.shape[0]
    units = act_b.shape[1]
    groups = lax.axis_size("tok")
    band = units // groups
    total_tokens = token_rows * groups
    wide_a = act_a.astype(jnp.float32)
    first_total = jnp.sum(wide_a, axis=0)
    first_square = jnp.sum(wide_a * wide_a, axis=0)
    piece = lax.all_gather(act_b, "unit", axis=0, tiled=True)
    product = contract_tokens(piece, act_a)
    wide_piece = piece.astype(jnp.float32)
    second_total = jnp.sum(wide_piece, axis=0)
    second_square = jnp.sum(wide_piece * wide_piece, axis=0)
    shares = lax.psum_scatter(product, "tok", scatter_dimension=0, tiled=True)
    first_all, first_square_all, second_all, second_square_all = lax.psum(
        (first_total, first_square, second_total, second_square), "tok"
    )
    offset = lax.axis_index("tok") * band
    second_own = lax.dynamic_slice_in_dim(second_all, offset, band, 0)
    second_square_own = lax.dynamic_slice_in_dim(second_square_all, offset, band, 0)
    mean_a = first_all / total_tokens
    var_a = first_square_all / total_tokens - mean_a * mean_a
    mean_b = second_own / total_tokens
    var_b = second_square_own / total_tokens - mean_b * mean_b
    centered = shares / total_tokens - mean_b[:, None] * mean_a[None, :]
    return centered / (jnp.sqrt(var_b + 1e-05)[:, None] * jnp.sqrt(var_a + 1e-05)[None, :])


def schedule(rings, parts):
    crosses, keeps = rings * parts, (rings - 1) * parts
    events = sorted(
        [((k + 0.25) / crosses, 0, k) for k in range(crosses)]
        + [((k + 1) / keeps, 1, k) for k in range(keeps)]
    )
    slots = [(kind, k) for _, kind, k in events] + [(1, keeps + i) for i in range(parts)]
    place = {slot: s for s, slot in enumerate(slots)}
    orders = []
    for r in range(rings):
        behind = lambda d: r if d > r else rings - 1 - r
        others = [d for d in range(rings) if d != r]
        orders.append(sorted(others, key=lambda d: (-abs(d - r), -behind(d), d)) + [r])
    done = [{} for _ in range(rings)]
    merges = [[0] * len(slots) for _ in range(rings)]
    for s in range(crosses + keeps):
        for r in range(rings):
            k = len(done[r])
            if k == keeps or place[1, k] > s or place[0, k] + 3 > s:
                continue
            d, i = orders[r][k // parts], k % parts
            before = r - 1 if d > r else r + 1
            if 0 <= before < rings and done[before].get((d, i), s) + 3 > s:
                continue
            done[r][d, i] = s
            merges[r][s] = k + 1
    complete = all(len(d) == keeps for d in done)
    return slots, orders, merges, complete


def pick(values, i):
    out = values[-1]
    for k in reversed(range(len(values) - 1)):
        if values[k] != values[k + 1] or not isinstance(out, (int, float)):
            out = jnp.where(i == k, values[k], out)
    return out


def pick_row(rows, r, i):
    out = None
    unique = []
    for row in rows:
        if row not in unique:
            unique.append(row)
    for row in unique:
        mine = pick(row, i)
        if out is None:
            out = mine
        else:
            here = functools.reduce(jnp.logical_or, [r == k for k in range(len(rows)) if rows[k] == row])
            out = jnp.where(here, mine, out)
    return out


def column(row):
    return jnp.transpose(jnp.broadcast_to(row, (LANES, LANES)))


def spread(square, total, share):
    return jnp.maximum(square - total * total * share, square * 1e-5 + 1e-30)


def encode(q):
    size = jnp.exp2(jnp.minimum(jnp.abs(q), 1.04) * SPAN - BASE)
    return jnp.where(q < 0, -size, size).astype(jnp.bfloat16)


def decode(code):
    y = code.astype(jnp.float32)
    size = jnp.log2(jnp.abs(y)) + BASE
    return jnp.where(y < 0, -size, size)


def kernel(groups, plan, a_hbm, b_hbm, out, a, g, held, cross_out, cross_in, far_out, far_in,
           sa_own, sa_near, sa_pair, sa_in, sa_run, sa_stat, sb_half, sb_mine, sb_near, sb_run, sb_in,
           a_sem, b_sem, px_send, px_recv, nx_send, nx_recv, fw_send, fw_recv,
           c_send, cb_send, c_recv, f_send, fb_send, f_recv,
           ca_send, ca_recv, fa_send, fa_recv):
    slots, orders, merges, _ = plan
    t = lax.axis_index("tok")
    u = lax.axis_index("unit")
    rows, units = b_hbm.shape
    tokens, own = a.shape
    band = units // groups
    parts = band // LANES
    rings = groups // 2
    crosses = rings * parts
    keeps = crosses - parts
    steps = len(slots)
    main = steps - parts
    bunch = steps // BUNCHES
    half = tokens // 2
    r = t // 2
    y = t % 2
    side = u // 2
    partner = u + 1 - 2 * (u % 2)
    across = (u + 2) % 4
    near = t + 1 - 2 * y
    shares = [1.0 / (2 * tokens * max(k, 1)) for k in range(rings + 1)]
    packed = [kind + 2 * (k // parts) + 2048 * (k % parts) for kind, k in slots]

    def slot(s):
        code = pick(packed, s)
        kind, p, i = code % 2, (code // 2) % 1024, code // 2048
        return kind, p, i

    def bound(p):
        return pick_row(orders, r, p)

    def columns(kind, p, i):
        owner = bound(p) * 2 + jnp.where(kind == 0, 1 - y, y)
        return pl.ds(pl.multiple_of(owner * band + i * LANES, LANES), LANES)

    def block(ref, who, cols):
        return ref.at[pl.ds(pl.multiple_of(who * rows, rows), rows), cols]

    def remote(src, dst, send, recv, tt, uu):
        return pltpu.make_async_remote_copy(
            src_ref=src, dst_ref=dst, send_sem=send, recv_sem=recv,
            device_id=(tt, uu), device_id_type=MESH)

    def to_partner(s, cols):
        return remote(b_hbm.at[:, cols], block(g, u, cols), px_send.at[0], px_recv.at[s // bunch], t, partner)

    def to_across(s, cols):
        return remote(b_hbm.at[:, cols], block(g, u, cols), nx_send.at[0], nx_recv.at[s % (2 * AHEAD)],
                      t, across)

    def forward(s, cols):
        return remote(block(g, across, cols), block(g, across, cols), fw_send.at[0],
                      fw_recv.at[2 * (s % 2)], t, partner)

    def piece(who, h, cols):
        size = rows // 2
        return g.at[pl.ds(pl.multiple_of(who * rows + h * size, size), size), cols]

    def last_across(i, h, cols):
        return remote(b_hbm.at[pl.ds(h * (rows // 2), rows // 2), cols], piece(u, h, cols),
                      nx_send.at[0], nx_recv.at[2 * AHEAD + 2 * i + h], t, across)

    def last_forward(s, h, cols):
        return remote(piece(across, h, cols), piece(across, h, cols), fw_send.at[0],
                      fw_recv.at[2 * (s % 2) + h], t, partner)

    def issue_across(s):
        cols = columns(*slot(s))

        @pl.when(s < main)
        def _():
            to_across(s, cols).start()

        @pl.when(jnp.logical_and(s >= main, s < steps))
        def _():
            for h in (0, 1):
                last_across(s - main, h, cols).start()

    def send_cross(k):
        return remote(cross_out.at[k], cross_in.at[k], c_send.at[0], c_recv.at[k], near, u)

    def send_cross_sums(k):
        return remote(sb_mine.at[k], sb_near.at[k], cb_send.at[0], c_recv.at[k], near, u)

    def both(sem):
        some = g.at[pl.ds(0, own + 16), pl.ds(0, LANES)]
        return pltpu.make_async_copy(some, some, sem)

    def send_far(k, j, tt):
        return remote(far_out.at[k], far_in.at[j], f_send.at[0], f_recv.at[j], tt, u)

    def send_far_sums(k, j, tt):
        return remote(sb_run.at[k], sb_in.at[j], fb_send.at[0], f_recv.at[j], tt, u)

    send_near_a = remote(sa_own, sa_near, ca_send.at[0], ca_recv.at[0], near, u)

    def send_run_a(way):
        tt = t + 2 if way == 0 else t - 2
        return remote(sa_run.at[way], sa_in.at[way], fa_send.at[way], fa_recv.at[way], tt, u)

    a_copy = pltpu.make_async_copy(a_hbm, a, a_sem)
    own_rows = pl.ds(pl.multiple_of(u * rows, rows), rows)
    b_copy = pltpu.make_async_copy(b_hbm, g.at[own_rows, :], b_sem)

    barrier = pltpu.get_barrier_semaphore()

    def greet(tt, uu):
        pl.semaphore_signal(barrier, inc=1, device_id=(tt, uu), device_id_type=MESH)

    greet(t, across)
    greet(t, partner)
    greet(near, u)

    @pl.when(r > 0)
    def _():
        greet(t - 2, u)

    @pl.when(r < rings - 1)
    def _():
        greet(t + 2, u)

    a_copy.start()
    b_copy.start()
    pl.semaphore_wait(barrier, 3 + jnp.where(r > 0, 1, 0) + jnp.where(r < rings - 1, 1, 0))

    @pl.loop(0, steps)
    def _(s):
        @pl.when(s < AHEAD)
        def _():
            issue_across(s)

        to_partner(s, columns(*slot(s))).start()

    a_copy.wait()
    b_copy.wait()
    chunk = 128

    def sum_rows(wide):
        wide = wide.astype(jnp.float32).reshape(wide.shape[0] // 8, 8, wide.shape[1])
        return jnp.sum(wide, axis=0), jnp.sum(wide * wide, axis=0)

    def body(i, carry):
        total, square = sum_rows(a[pl.ds(pl.multiple_of(i * chunk, chunk), chunk), :])
        return carry[0] + total, carry[1] + square

    zero = jnp.zeros((8, own), jnp.float32)
    total, square = lax.fori_loop(0, tokens // chunk, body, (zero, zero))
    sa_own[...] = jnp.zeros((8, own), jnp.float32)
    sa_own[0:1, :] = jnp.sum(total, axis=0, keepdims=True)
    sa_own[1:2, :] = jnp.sum(square, axis=0, keepdims=True)
    send_near_a.start()

    def tiles():
        return [slice(c * LANES, (c + 1) * LANES) for c in range(own // LANES)]

    def early(hold, cols):
        mine = pl.ds(pl.multiple_of(side * half, half), half)
        lhs = g[mine, cols]
        held[hold] = contract_tokens(lhs, a[mine, :])
        total, square = sum_rows(lhs)
        sb_half[0] = total
        sb_half[1] = square

    def part(hold, start, size, cols):
        some = pl.ds(pl.multiple_of(start, size), size)
        lhs = g[some, cols]
        held[hold] = held[hold] + contract_tokens(lhs, a[some, :])
        total, square = sum_rows(lhs)
        sb_half[0] = sb_half[0] + total
        sb_half[1] = sb_half[1] + square

    def finish_sums(k):
        sb_mine[k] = jnp.zeros((8, LANES), jnp.float32)
        sb_mine[k, 0:1, :] = jnp.sum(sb_half[0], axis=0, keepdims=True)
        sb_mine[k, 1:2, :] = jnp.sum(sb_half[1], axis=0, keepdims=True)

    def late(hold, k, cols):
        theirs = pl.ds(pl.multiple_of((1 - side) * half, half), half)
        lhs = g[theirs, cols]
        held[hold] = held[hold] + contract_tokens(lhs, a[theirs, :])
        total, square = sum_rows(lhs)
        sb_half[0] = sb_half[0] + total
        sb_half[1] = sb_half[1] + square
        finish_sums(k)

    def put(target, k, hold, sb, sa, share):
        tb, qb = sb[0:1, :], sb[1:2, :]
        tb_col = column(tb * share)
        scale_col = column(lax.rsqrt(spread(qb, tb, share)))
        for cols in tiles():
            ta = sa[0:1, cols]
            scale = lax.rsqrt(spread(sa[1:2, cols], ta, share))
            q = (held[hold, :, cols] - tb_col * ta) * (scale_col * scale)
            target[k, :, cols] = encode(q)

    def take(hold, source, k, sb, sa, share):
        tb, qb = sb[0:1, :], sb[1:2, :]
        tb_col = column(tb * share)
        norm_col = column(jnp.sqrt(spread(qb, tb, share)) * (1.0 / SPAN))
        for cols in tiles():
            ta = sa[0:1, cols]
            norm = jnp.sqrt(spread(sa[1:2, cols], ta, share))
            held[hold, :, cols] = held[hold, :, cols] + (
                decode(source[k, :, cols]) * (norm_col * norm) + tb_col * ta)

    def take_near(k):
        both(c_recv.at[k]).wait()
        take(k, cross_in, k, sb_near.at[k], sa_near, 1.0 / tokens)

    def take_far(way, k, j):
        both(f_recv.at[j]).wait()
        count = jnp.where(way == 0, r, rings - 1 - r)
        take(k, far_in, j, sb_in.at[j], sa_in.at[way], pick(shares, count))

    def route(k):
        p, i = k // parts, k % parts
        d = bound(p)
        way = jnp.where(d > r, 0, 1)
        count = jnp.where(way == 0, r, rings - 1 - r)
        distance = jnp.where(way == 0, d - r, r - d)
        return way, count, (way * (rings - 1) + distance) * parts + i

    def collect(k):
        way, count, j = route(k)
        take_near(k)

        @pl.when(count > 0)
        def _():
            take_far(way, k, j)

    def pass_on(k):
        way, count, j = route(k)
        sb_run[k] = sb_mine[crosses + k] + sb_near[k]

        @pl.when(count > 0)
        def _():
            sb_run[k] = sb_run[k] + sb_in[j]

        put(far_out, k, k, sb_run.at[k], sa_run.at[way], pick(shares, count + 1))
        tt = t + 2 - 4 * way
        send_far(k, j - parts, tt).start()
        send_far_sums(k, j - parts, tt).start()

    def exchange_a(s):
        @pl.when(s == 1)
        def _():
            send_near_a.wait_recv()
            sa_pair[...] = sa_own[...] + sa_near[...]

        for way, ready in ((0, r + 1), (1, rings - r)):
            first = (r == 0) if way == 0 else (r == rings - 1)
            final = (r == rings - 1) if way == 0 else (r == 0)

            @pl.when(jnp.logical_and(s == ready, first))
            def _():
                sa_in[way] = jnp.zeros((8, own), jnp.float32)
                sa_run[way] = sa_pair[...]

            @pl.when(jnp.logical_and(s == ready, jnp.logical_not(first)))
            def _():
                send_run_a(way).wait_recv()
                sa_run[way] = sa_pair[...] + sa_in[way]

            @pl.when(jnp.logical_and(s == ready, jnp.logical_not(final)))
            def _():
                send_run_a(way).start()

    def partner_ready(s):
        @pl.when(s % bunch == 0)
        def _():
            to_partner(s, pl.ds(0, LANES * bunch)).wait_recv()

    @pl.loop(0, main)
    def _(s):
        kind, p, i = slot(s)
        cols = columns(kind, p, i)
        k = p * parts + i
        hold = jnp.where(kind == 0, crosses, k)
        partner_ready(s)
        early(hold, cols)
        to_across(s, cols).wait_recv()
        forward(s, cols).start()
        issue_across(s + AHEAD)
        exchange_a(s)
        pair = pick_row(merges, r, s)

        @pl.when(pair > 0)
        def _():
            collect(pair - 1)

        forward(s, cols).wait_recv()
        late(hold, kind * crosses + k, cols)

        @pl.when(kind == 0)
        def _():
            put(cross_out, k, hold, sb_mine.at[k], sa_own, 1.0 / tokens)
            send_cross(k).start()
            send_cross_sums(k).start()

        @pl.when(pair > 0)
        def _():
            pass_on(pair - 1)

    whole_a = sa_pair[...] + sa_in[0] + sa_in[1]
    total_tokens = tokens * groups
    mean_a = whole_a[0:1, :] * (1.0 / total_tokens)
    var_a = whole_a[1:2, :] * (1.0 / total_tokens) - mean_a * mean_a
    sa_stat[0:1, :] = mean_a
    sa_stat[1:2, :] = 1.0 / jnp.sqrt(var_a + 1e-05)

    @pl.loop(0, parts)
    def _(i):
        s = main + i
        k = keeps + i
        cols = pl.ds(pl.multiple_of(t * band + i * LANES, LANES), LANES)
        partner_ready(s)
        early(k, cols)
        for h in (0, 1):
            last_across(i, h, cols).wait_recv()
            last_forward(s, h, cols).start()
        part(k, across * rows, rows, cols)
        take_near(k)
        sb_half[2] = sb_near[k]
        for way, some in ((0, r > 0), (1, r < rings - 1)):
            @pl.when(some)
            def _():
                j = way * (rings - 1) * parts + i
                take_far(way, k, j)
                sb_half[2] = sb_half[2] + sb_in[j]

        for h in (0, 1):
            last_forward(s, h, cols).wait_recv()
            part(k, (across + 1 - 2 * (across % 2)) * rows + h * (rows // 2), rows // 2, cols)
        finish_sums(crosses + k)
        whole_b = sb_half[2] + sb_mine[crosses + k]
        mean_b = whole_b[0:1, :] * (1.0 / total_tokens)
        var_b = whole_b[1:2, :] * (1.0 / total_tokens) - mean_b * mean_b
        mean_col = column(mean_b)
        inv_col = column(1.0 / jnp.sqrt(var_b + 1e-05))
        lanes = pl.ds(pl.multiple_of(i * LANES, LANES), LANES)
        for c in tiles():
            centered = held[k, :, c] * (1.0 / total_tokens) - mean_col * sa_stat[0:1, c]
            out[lanes, c] = centered * (inv_col * sa_stat[1:2, c])

    send_near_a.wait_send()

    @pl.when(r < rings - 1)
    def _():
        send_run_a(0).wait_send()

    @pl.when(r > 0)
    def _():
        send_run_a(1).wait_send()

    own_b = g.at[own_rows, :]
    remote(b_hbm, own_b, nx_send.at[0], nx_recv.at[0], t, across).wait_send()
    remote(b_hbm, own_b, px_send.at[0], px_recv.at[0], t, partner).wait_send()
    remote(own_b, own_b, fw_send.at[0], fw_recv.at[0], t, partner).wait_send()
    remote(cross_out, cross_in, c_send.at[0], c_recv.at[0], near, u).wait_send()
    remote(sb_near, sb_near, cb_send.at[0], c_recv.at[0], near, u).wait_send()
    remote(far_out, far_out, f_send.at[0], f_recv.at[0], near, u).wait_send()
    remote(sb_run, sb_run, fb_send.at[0], f_recv.at[0], near, u).wait_send()


def fused(groups, plan, act_a, act_b):
    tokens, own = act_a.shape
    rows, units = act_b.shape
    band = units // groups
    parts = band // LANES
    rings = groups // 2
    crosses = rings * parts
    keeps = crosses - parts
    steps = 2 * crosses
    dma = lambda n: pltpu.SemaphoreType.DMA((n,))
    bf16 = lambda *shape: pltpu.VMEM(shape, jnp.bfloat16)
    f32 = lambda *shape: pltpu.VMEM(shape, jnp.float32)
    return pl.pallas_call(
        functools.partial(kernel, groups, plan),
        out_shape=jax.ShapeDtypeStruct((band, own), jnp.float32),
        in_specs=[pl.BlockSpec(memory_space=pltpu.HBM)] * 2,
        out_specs=pl.BlockSpec(memory_space=pltpu.VMEM),
        scratch_shapes=[
            bf16(tokens, own),
            bf16(tokens, units),
            f32(crosses + 1, LANES, own),
            bf16(crosses, LANES, own),
            bf16(crosses, LANES, own),
            bf16(keeps, LANES, own),
            bf16(2 * keeps, LANES, own),
            f32(8, own), f32(8, own), f32(8, own),
            f32(2, 8, own), f32(2, 8, own), f32(8, own),
            f32(3, 8, LANES),
            f32(2 * crosses, 8, LANES), f32(crosses, 8, LANES),
            f32(keeps, 8, LANES), f32(2 * keeps, 8, LANES),
            pltpu.SemaphoreType.DMA, pltpu.SemaphoreType.DMA,
            dma(1), dma(BUNCHES),
            dma(1), dma(2 * AHEAD + 2 * parts),
            dma(1), dma(4),
            dma(1), dma(1), dma(crosses),
            dma(1), dma(1), dma(2 * keeps),
            dma(1), dma(1),
            dma(2), dma(2),
        ],
        compiler_params=pltpu.CompilerParams(
            collective_id=0, has_side_effects=True, vmem_limit_bytes=52000 * 1024
        ),
        name="gather_correlate",
    )(act_a, act_b)


def solution(mesh):
    groups, split = mesh.shape["tok"], mesh.shape["unit"]

    def per_device(act_a, act_b):
        band = act_b.shape[1] // groups
        whole = act_a.shape[0] % 256 == 0 and act_a.shape[1] % LANES == 0
        if split == 4 and groups % 2 == 0 and groups > 4 and band % LANES == 0 and whole:
            plan = schedule(groups // 2, band // LANES)
            if plan[-1] and len(plan[0]) % BUNCHES == 0:
                return fused(groups, plan, act_a, act_b)
        return plain(act_a, act_b)

    placed = (P("tok", "unit"), P(("tok", "unit"), None))
    return jax.shard_map(
        per_device, mesh=mesh, in_specs=placed, out_specs=P("tok", "unit"), check_vma=False
    )
```

```python
import functools

import jax
import jax.numpy as jnp
from jax import lax
from jax.experimental import pallas as pl
from jax.experimental.pallas import tpu as pltpu
from jax.sharding import PartitionSpec as P

MESH = pl.DeviceIdType.MESH
LANES = 128
SPAN = 240.0
BASE = 120.0
AHEAD = 4
BUNCHES = 4


def contract_tokens(left, right):
    return lax.dot_general(
        left, right, (((0,), (0,)), ((), ())), preferred_element_type=jnp.float32
    )


def plain(act_a, act_b):
    token_rows = act_a.shape[0]
    units = act_b.shape[1]
    groups = lax.axis_size("tok")
    band = units // groups
    total_tokens = token_rows * groups
    wide_a = act_a.astype(jnp.float32)
    first_total = jnp.sum(wide_a, axis=0)
    first_square = jnp.sum(wide_a * wide_a, axis=0)
    piece = lax.all_gather(act_b, "unit", axis=0, tiled=True)
    product = contract_tokens(piece, act_a)
    wide_piece = piece.astype(jnp.float32)
    second_total = jnp.sum(wide_piece, axis=0)
    second_square = jnp.sum(wide_piece * wide_piece, axis=0)
    shares = lax.psum_scatter(product, "tok", scatter_dimension=0, tiled=True)
    first_all, first_square_all, second_all, second_square_all = lax.psum(
        (first_total, first_square, second_total, second_square), "tok"
    )
    offset = lax.axis_index("tok") * band
    second_own = lax.dynamic_slice_in_dim(second_all, offset, band, 0)
    second_square_own = lax.dynamic_slice_in_dim(second_square_all, offset, band, 0)
    mean_a = first_all / total_tokens
    var_a = first_square_all / total_tokens - mean_a * mean_a
    mean_b = second_own / total_tokens
    var_b = second_square_own / total_tokens - mean_b * mean_b
    centered = shares / total_tokens - mean_b[:, None] * mean_a[None, :]
    return centered / (jnp.sqrt(var_b + 1e-05)[:, None] * jnp.sqrt(var_a + 1e-05)[None, :])


def schedule(rings, parts):
    crosses, keeps = rings * parts, (rings - 1) * parts
    events = sorted(
        [((k + 0.25) / crosses, 0, k) for k in range(crosses)]
        + [((k + 1) / keeps, 1, k) for k in range(keeps)]
    )
    slots = [(kind, k) for _, kind, k in events] + [(1, keeps + i) for i in range(parts)]
    place = {slot: s for s, slot in enumerate(slots)}
    orders = []
    for r in range(rings):
        behind = lambda d: r if d > r else rings - 1 - r
        others = [d for d in range(rings) if d != r]
        orders.append(sorted(others, key=lambda d: (-abs(d - r), -behind(d), d)) + [r])
    done = [{} for _ in range(rings)]
    merges = [[0] * len(slots) for _ in range(rings)]
    for s in range(crosses + keeps):
        for r in range(rings):
            k = len(done[r])
            if k == keeps or place[1, k] > s or place[0, k] + 3 > s:
                continue
            d, i = orders[r][k // parts], k % parts
            before = r - 1 if d > r else r + 1
            if 0 <= before < rings and done[before].get((d, i), s) + 3 > s:
                continue
            done[r][d, i] = s
            merges[r][s] = k + 1
    complete = all(len(d) == keeps for d in done)
    return slots, orders, merges, complete


def pick(values, i):
    out = values[-1]
    for k in reversed(range(len(values) - 1)):
        if values[k] != values[k + 1] or not isinstance(out, (int, float)):
            out = jnp.where(i == k, values[k], out)
    return out


def pick_row(rows, r, i):
    out = None
    unique = []
    for row in rows:
        if row not in unique:
            unique.append(row)
    for row in unique:
        mine = pick(row, i)
        if out is None:
            out = mine
        else:
            here = functools.reduce(jnp.logical_or, [r == k for k in range(len(rows)) if rows[k] == row])
            out = jnp.where(here, mine, out)
    return out


def column(row):
    return jnp.transpose(jnp.broadcast_to(row, (LANES, LANES)))


def spread(square, total, share):
    return jnp.maximum(square - total * total * share, square * 1e-5 + 1e-30)


def encode(q):
    size = jnp.exp2(jnp.minimum(jnp.abs(q), 1.03) * SPAN - BASE)
    return jnp.where(q < 0, -size, size).astype(jnp.bfloat16)


def decode(code):
    y = code.astype(jnp.float32)
    size = jnp.log2(jnp.abs(y)) + BASE
    return jnp.where(y < 0, -size, size)


def kernel(groups, plan, a_hbm, b_hbm, out, a, g, held, cross_out, cross_in, far_out, far_in,
           sa_own, sa_near, sa_pair, sa_in, sa_run, sa_stat, sb_half, sb_mine, sb_near, sb_run, sb_in,
           a_sem, b_sem, px_send, px_recv, nx_send, nx_recv, fw_send, fw_recv,
           c_send, cb_send, c_recv, f_send, fb_send, f_recv,
           ca_send, ca_recv, fa_send, fa_recv, ready, go):
    slots, orders, merges, _ = plan
    t = lax.axis_index("tok")
    u = lax.axis_index("unit")
    rows, units = b_hbm.shape
    tokens, own = a.shape
    band = units // groups
    parts = band // LANES
    rings = groups // 2
    crosses = rings * parts
    keeps = crosses - parts
    steps = len(slots)
    main = steps - parts
    bunch = steps // BUNCHES
    half = tokens // 2
    r = t // 2
    y = t % 2
    side = u // 2
    partner = u + 1 - 2 * (u % 2)
    across = (u + 2) % 4
    near = t + 1 - 2 * y
    shares = [1.0 / (2 * tokens * max(k, 1)) for k in range(rings + 1)]
    packed = [kind + 2 * (k // parts) + 2048 * (k % parts) for kind, k in slots]

    def slot(s):
        code = pick(packed, s)
        kind, p, i = code % 2, (code // 2) % 1024, code // 2048
        return kind, p, i

    def bound(p):
        return pick_row(orders, r, p)

    def columns(kind, p, i):
        owner = bound(p) * 2 + jnp.where(kind == 0, 1 - y, y)
        return pl.ds(pl.multiple_of(owner * band + i * LANES, LANES), LANES)

    def block(ref, who, cols):
        return ref.at[pl.ds(pl.multiple_of(who * rows, rows), rows), cols]

    def remote(src, dst, send, recv, tt, uu):
        return pltpu.make_async_remote_copy(
            src_ref=src, dst_ref=dst, send_sem=send, recv_sem=recv,
            device_id=(tt, uu), device_id_type=MESH)

    def to_partner(s, cols):
        return remote(b_hbm.at[:, cols], block(g, u, cols), px_send.at[0], px_recv.at[s // bunch], t, partner)

    def to_across(s, cols):
        return remote(block(g, u, cols), block(g, u, cols), nx_send.at[0], nx_recv.at[s % (2 * AHEAD)],
                      t, across)

    def forward(s, cols):
        return remote(block(g, across, cols), block(g, across, cols), fw_send.at[0],
                      fw_recv.at[2 * (s % 2)], t, partner)

    def piece(who, h, cols):
        size = rows // 2
        return g.at[pl.ds(pl.multiple_of(who * rows + h * size, size), size), cols]

    def last_across(i, h, cols):
        return remote(piece(u, h, cols), piece(u, h, cols),
                      nx_send.at[0], nx_recv.at[2 * AHEAD + 2 * i + h], t, across)

    def last_forward(s, h, cols):
        return remote(piece(across, h, cols), piece(across, h, cols), fw_send.at[0],
                      fw_recv.at[2 * (s % 2) + h], t, partner)

    def issue_across(s):
        cols = columns(*slot(s))

        @pl.when(s < main)
        def _():
            to_across(s, cols).start()

        @pl.when(jnp.logical_and(s >= main, s < steps))
        def _():
            for h in (0, 1):
                last_across(s - main, h, cols).start()

    def send_cross(k):
        return remote(cross_out.at[k], cross_in.at[k], c_send.at[0], c_recv.at[k], near, u)

    def send_cross_sums(k):
        return remote(sb_mine.at[k], sb_near.at[k], cb_send.at[0], c_recv.at[k], near, u)

    def both(sem):
        some = g.at[pl.ds(0, own + 16), pl.ds(0, LANES)]
        return pltpu.make_async_copy(some, some, sem)

    def send_far(k, j, tt):
        return remote(far_out.at[k], far_in.at[j], f_send.at[0], f_recv.at[j], tt, u)

    def send_far_sums(k, j, tt):
        return remote(sb_run.at[k], sb_in.at[j], fb_send.at[0], f_recv.at[j], tt, u)

    send_near_a = remote(sa_own, sa_near, ca_send.at[0], ca_recv.at[0], near, u)

    def send_run_a(way):
        tt = t + 2 if way == 0 else t - 2
        return remote(sa_run.at[way], sa_in.at[way], fa_send.at[way], fa_recv.at[way], tt, u)

    a_copy = pltpu.make_async_copy(a_hbm, a, a_sem)
    own_rows = pl.ds(pl.multiple_of(u * rows, rows), rows)

    def b_copy(s):
        cols = columns(*slot(s))
        return pltpu.make_async_copy(
            b_hbm.at[:, cols], g.at[own_rows, cols], b_sem.at[jnp.where(s == 0, 0, jnp.where(s < AHEAD, 1, 2))])

    def b_wait(which, count):
        cols = pl.ds(0, LANES * count)
        pltpu.make_async_copy(b_hbm.at[:, cols], g.at[own_rows, cols], b_sem.at[which]).wait()

    barrier = pltpu.get_barrier_semaphore()

    early_core = u % 2 == 0
    wide_core = u % 2 == 1
    peers = 1 + jnp.where(r > 0, 1, 0) + jnp.where(r < rings - 1, 1, 0)

    def tell(sem, tt, uu):
        pl.semaphore_signal(sem, inc=1, device_id=(tt, uu), device_id_type=MESH)

    def tell_peers(sem):
        tell(sem, near, u)

        @pl.when(r > 0)
        def _():
            tell(sem, t - 2, u)

        @pl.when(r < rings - 1)
        def _():
            tell(sem, t + 2, u)

    tell(barrier, t, across)
    tell(barrier, t, partner)

    @pl.when(wide_core)
    def _():
        tell_peers(barrier)

    @pl.loop(0, AHEAD)
    def _(s):
        b_copy(s).start()

    a_copy.start()
    pl.semaphore_wait(barrier, 2 + jnp.where(wide_core, peers, 0))

    @pl.when(wide_core)
    def _():
        tell_peers(ready)

    b_wait(0, 1)
    issue_across(jnp.int32(0))
    b_wait(1, AHEAD - 1)

    @pl.loop(1, AHEAD)
    def _(s):
        issue_across(s)

    @pl.loop(0, steps)
    def _(s):
        to_partner(s, columns(*slot(s))).start()

        @pl.when(s >= AHEAD)
        def _():
            b_copy(s).start()

    b_wait(2, steps - AHEAD)
    a_copy.wait()
    chunk = 128

    def sum_rows(wide):
        wide = wide.astype(jnp.float32).reshape(wide.shape[0] // 8, 8, wide.shape[1])
        return jnp.sum(wide, axis=0), jnp.sum(wide * wide, axis=0)

    def body(i, carry):
        total, square = sum_rows(a[pl.ds(pl.multiple_of(i * chunk, chunk), chunk), :])
        return carry[0] + total, carry[1] + square

    zero = jnp.zeros((8, own), jnp.float32)
    total, square = lax.fori_loop(0, tokens // chunk, body, (zero, zero))
    sa_own[...] = jnp.zeros((8, own), jnp.float32)
    sa_own[0:1, :] = jnp.sum(total, axis=0, keepdims=True)
    sa_own[1:2, :] = jnp.sum(square, axis=0, keepdims=True)

    @pl.when(wide_core)
    def _():
        pl.semaphore_wait(ready, peers)
        tell(go, t, partner)

    @pl.when(early_core)
    def _():
        pl.semaphore_wait(go, 1)

    send_near_a.start()

    def tiles():
        return [slice(c * LANES, (c + 1) * LANES) for c in range(own // LANES)]

    def early(hold, cols):
        mine = pl.ds(pl.multiple_of(side * half, half), half)
        lhs = g[mine, cols]
        held[hold] = contract_tokens(lhs, a[mine, :])
        total, square = sum_rows(lhs)
        sb_half[0] = total
        sb_half[1] = square

    def part(hold, start, size, cols):
        some = pl.ds(pl.multiple_of(start, size), size)
        lhs = g[some, cols]
        held[hold] = held[hold] + contract_tokens(lhs, a[some, :])
        total, square = sum_rows(lhs)
        sb_half[0] = sb_half[0] + total
        sb_half[1] = sb_half[1] + square

    def finish_sums(k):
        sb_mine[k] = jnp.zeros((8, LANES), jnp.float32)
        sb_mine[k, 0:1, :] = jnp.sum(sb_half[0], axis=0, keepdims=True)
        sb_mine[k, 1:2, :] = jnp.sum(sb_half[1], axis=0, keepdims=True)

    def put(target, k, hold, sb, sa, share):
        tb, qb = sb[0:1, :], sb[1:2, :]
        tb_col = column(tb * share)
        scale_col = column(lax.rsqrt(spread(qb, tb, share)))
        for cols in tiles():
            ta = sa[0:1, cols]
            scale = lax.rsqrt(spread(sa[1:2, cols], ta, share))
            q = (held[hold, :, cols] - tb_col * ta) * (scale_col * scale)
            target[k, :, cols] = encode(q)

    def take(hold, source, k, sb, sa, share):
        tb, qb = sb[0:1, :], sb[1:2, :]
        tb_col = column(tb * share)
        norm_col = column(jnp.sqrt(spread(qb, tb, share)) * (1.0 / SPAN))
        for cols in tiles():
            ta = sa[0:1, cols]
            norm = jnp.sqrt(spread(sa[1:2, cols], ta, share))
            held[hold, :, cols] = held[hold, :, cols] + (
                decode(source[k, :, cols]) * (norm_col * norm) + tb_col * ta)

    def take_near(k):
        both(c_recv.at[k]).wait()
        take(k, cross_in, k, sb_near.at[k], sa_near, 1.0 / tokens)

    def take_far(way, k, j):
        both(f_recv.at[j]).wait()
        count = jnp.where(way == 0, r, rings - 1 - r)
        take(k, far_in, j, sb_in.at[j], sa_in.at[way], pick(shares, count))

    def route(k):
        p, i = k // parts, k % parts
        d = bound(p)
        way = jnp.where(d > r, 0, 1)
        count = jnp.where(way == 0, r, rings - 1 - r)
        distance = jnp.where(way == 0, d - r, r - d)
        return way, count, (way * (rings - 1) + distance) * parts + i

    def collect(k):
        way, count, j = route(k)
        take_near(k)

        @pl.when(count > 0)
        def _():
            take_far(way, k, j)

    def pass_on(k):
        way, count, j = route(k)
        sb_run[k] = sb_mine[crosses + k] + sb_near[k]

        @pl.when(count > 0)
        def _():
            sb_run[k] = sb_run[k] + sb_in[j]

        put(far_out, k, k, sb_run.at[k], sa_run.at[way], pick(shares, count + 1))
        tt = t + 2 - 4 * way
        send_far(k, j - parts, tt).start()
        send_far_sums(k, j - parts, tt).start()

    def exchange_a(s):
        @pl.when(s == 1)
        def _():
            send_near_a.wait_recv()
            sa_pair[...] = sa_own[...] + sa_near[...]

        for way, ready in ((0, r + 1), (1, rings - r)):
            first = (r == 0) if way == 0 else (r == rings - 1)
            final = (r == rings - 1) if way == 0 else (r == 0)

            @pl.when(jnp.logical_and(s == ready, first))
            def _():
                sa_in[way] = jnp.zeros((8, own), jnp.float32)
                sa_run[way] = sa_pair[...]

            @pl.when(jnp.logical_and(s == ready, jnp.logical_not(first)))
            def _():
                send_run_a(way).wait_recv()
                sa_run[way] = sa_pair[...] + sa_in[way]

            @pl.when(jnp.logical_and(s == ready, jnp.logical_not(final)))
            def _():
                send_run_a(way).start()

    def partner_ready(s):
        @pl.when(s % bunch == 0)
        def _():
            to_partner(s, pl.ds(0, LANES * bunch)).wait_recv()

    @pl.loop(0, main)
    def _(s):
        kind, p, i = slot(s)
        cols = columns(kind, p, i)
        k = p * parts + i
        hold = jnp.where(kind == 0, crosses, k)
        partner_ready(s)
        early(hold, cols)
        to_across(s, cols).wait_recv()
        forward(s, cols).start()
        issue_across(s + AHEAD)
        exchange_a(s)
        pair = pick_row(merges, r, s)

        @pl.when(pair > 0)
        def _():
            collect(pair - 1)

        part(hold, across * rows, rows, cols)
        forward(s, cols).wait_recv()
        part(hold, (across + 1 - 2 * (across % 2)) * rows, rows, cols)
        finish_sums(kind * crosses + k)

        @pl.when(kind == 0)
        def _():
            put(cross_out, k, hold, sb_mine.at[k], sa_own, 1.0 / tokens)
            send_cross(k).start()
            send_cross_sums(k).start()

        @pl.when(pair > 0)
        def _():
            pass_on(pair - 1)

    whole_a = sa_pair[...] + sa_in[0] + sa_in[1]
    total_tokens = tokens * groups
    mean_a = whole_a[0:1, :] * (1.0 / total_tokens)
    var_a = whole_a[1:2, :] * (1.0 / total_tokens) - mean_a * mean_a
    sa_stat[0:1, :] = mean_a
    sa_stat[1:2, :] = 1.0 / jnp.sqrt(var_a + 1e-05)

    @pl.loop(0, parts)
    def _(i):
        s = main + i
        k = keeps + i
        cols = pl.ds(pl.multiple_of(t * band + i * LANES, LANES), LANES)
        partner_ready(s)
        early(k, cols)
        for h in (0, 1):
            last_across(i, h, cols).wait_recv()
            last_forward(s, h, cols).start()
        part(k, across * rows, rows, cols)
        take_near(k)
        sb_half[2] = sb_near[k]
        for way, some in ((0, r > 0), (1, r < rings - 1)):
            @pl.when(some)
            def _():
                j = way * (rings - 1) * parts + i
                take_far(way, k, j)
                sb_half[2] = sb_half[2] + sb_in[j]

        for h in (0, 1):
            last_forward(s, h, cols).wait_recv()
            part(k, (across + 1 - 2 * (across % 2)) * rows + h * (rows // 2), rows // 2, cols)
        finish_sums(crosses + k)
        whole_b = sb_half[2] + sb_mine[crosses + k]
        mean_b = whole_b[0:1, :] * (1.0 / total_tokens)
        var_b = whole_b[1:2, :] * (1.0 / total_tokens) - mean_b * mean_b
        mean_col = column(mean_b)
        inv_col = column(1.0 / jnp.sqrt(var_b + 1e-05))
        lanes = pl.ds(pl.multiple_of(i * LANES, LANES), LANES)
        for c in tiles():
            centered = held[k, :, c] * (1.0 / total_tokens) - mean_col * sa_stat[0:1, c]
            out[lanes, c] = centered * (inv_col * sa_stat[1:2, c])

    send_near_a.wait_send()

    @pl.when(r < rings - 1)
    def _():
        send_run_a(0).wait_send()

    @pl.when(r > 0)
    def _():
        send_run_a(1).wait_send()

    own_b = g.at[own_rows, :]
    remote(own_b, own_b, nx_send.at[0], nx_recv.at[0], t, across).wait_send()
    remote(b_hbm, own_b, px_send.at[0], px_recv.at[0], t, partner).wait_send()
    remote(own_b, own_b, fw_send.at[0], fw_recv.at[0], t, partner).wait_send()
    remote(cross_out, cross_in, c_send.at[0], c_recv.at[0], near, u).wait_send()
    remote(sb_near, sb_near, cb_send.at[0], c_recv.at[0], near, u).wait_send()
    remote(far_out, far_out, f_send.at[0], f_recv.at[0], near, u).wait_send()
    remote(sb_run, sb_run, fb_send.at[0], f_recv.at[0], near, u).wait_send()


def fused(groups, plan, act_a, act_b):
    tokens, own = act_a.shape
    rows, units = act_b.shape
    band = units // groups
    parts = band // LANES
    rings = groups // 2
    crosses = rings * parts
    keeps = crosses - parts
    steps = 2 * crosses
    dma = lambda n: pltpu.SemaphoreType.DMA((n,))
    bf16 = lambda *shape: pltpu.VMEM(shape, jnp.bfloat16)
    f32 = lambda *shape: pltpu.VMEM(shape, jnp.float32)
    return pl.pallas_call(
        functools.partial(kernel, groups, plan),
        out_shape=jax.ShapeDtypeStruct((band, own), jnp.float32),
        in_specs=[pl.BlockSpec(memory_space=pltpu.HBM)] * 2,
        out_specs=pl.BlockSpec(memory_space=pltpu.VMEM),
        scratch_shapes=[
            bf16(tokens, own),
            bf16(tokens, units),
            f32(crosses + 1, LANES, own),
            bf16(crosses, LANES, own),
            bf16(crosses, LANES, own),
            bf16(keeps, LANES, own),
            bf16(2 * keeps, LANES, own),
            f32(8, own), f32(8, own), f32(8, own),
            f32(2, 8, own), f32(2, 8, own), f32(8, own),
            f32(3, 8, LANES),
            f32(2 * crosses, 8, LANES), f32(crosses, 8, LANES),
            f32(keeps, 8, LANES), f32(2 * keeps, 8, LANES),
            pltpu.SemaphoreType.DMA, dma(3),
            dma(1), dma(BUNCHES),
            dma(1), dma(2 * AHEAD + 2 * parts),
            dma(1), dma(4),
            dma(1), dma(1), dma(crosses),
            dma(1), dma(1), dma(2 * keeps),
            dma(1), dma(1),
            dma(2), dma(2),
            pltpu.SemaphoreType.REGULAR, pltpu.SemaphoreType.REGULAR,
        ],
        compiler_params=pltpu.CompilerParams(
            collective_id=0, has_side_effects=True, vmem_limit_bytes=52000 * 1024
        ),
        name="gather_correlate",
    )(act_a, act_b)


def solution(mesh):
    groups, split = mesh.shape["tok"], mesh.shape["unit"]

    def per_device(act_a, act_b):
        band = act_b.shape[1] // groups
        whole = act_a.shape[0] % 256 == 0 and act_a.shape[1] % LANES == 0
        if split == 4 and groups % 2 == 0 and groups > 4 and band % LANES == 0 and whole:
            plan = schedule(groups // 2, band // LANES)
            if plan[-1] and len(plan[0]) % BUNCHES == 0:
                return fused(groups, plan, act_a, act_b)
        return plain(act_a, act_b)

    placed = (P("tok", "unit"), P(("tok", "unit"), None))
    return jax.shard_map(
        per_device, mesh=mesh, in_specs=placed, out_specs=P("tok", "unit"), check_vma=False
    )
```

```python
import functools

import jax
import jax.numpy as jnp
from jax import lax
from jax.experimental import pallas as pl
from jax.experimental.pallas import tpu as pltpu
from jax.sharding import PartitionSpec as P

MESH = pl.DeviceIdType.MESH
LANES = 128
SPAN = 244.0
BASE = 122.0
AHEAD = 4
BUNCHES = 4


def contract_tokens(left, right):
    return lax.dot_general(
        left, right, (((0,), (0,)), ((), ())), preferred_element_type=jnp.float32
    )


def plain(act_a, act_b):
    token_rows = act_a.shape[0]
    units = act_b.shape[1]
    groups = lax.axis_size("tok")
    band = units // groups
    total_tokens = token_rows * groups
    wide_a = act_a.astype(jnp.float32)
    first_total = jnp.sum(wide_a, axis=0)
    first_square = jnp.sum(wide_a * wide_a, axis=0)
    piece = lax.all_gather(act_b, "unit", axis=0, tiled=True)
    product = contract_tokens(piece, act_a)
    wide_piece = piece.astype(jnp.float32)
    second_total = jnp.sum(wide_piece, axis=0)
    second_square = jnp.sum(wide_piece * wide_piece, axis=0)
    shares = lax.psum_scatter(product, "tok", scatter_dimension=0, tiled=True)
    first_all, first_square_all, second_all, second_square_all = lax.psum(
        (first_total, first_square, second_total, second_square), "tok"
    )
    offset = lax.axis_index("tok") * band
    second_own = lax.dynamic_slice_in_dim(second_all, offset, band, 0)
    second_square_own = lax.dynamic_slice_in_dim(second_square_all, offset, band, 0)
    mean_a = first_all / total_tokens
    var_a = first_square_all / total_tokens - mean_a * mean_a
    mean_b = second_own / total_tokens
    var_b = second_square_own / total_tokens - mean_b * mean_b
    centered = shares / total_tokens - mean_b[:, None] * mean_a[None, :]
    return centered / (jnp.sqrt(var_b + 1e-05)[:, None] * jnp.sqrt(var_a + 1e-05)[None, :])


def schedule(rings, parts):
    crosses, keeps = rings * parts, (rings - 1) * parts
    events = sorted(
        [((k + 0.25) / crosses, 0, k) for k in range(crosses)]
        + [((k + 1) / keeps, 1, k) for k in range(keeps)]
    )
    slots = [(kind, k) for _, kind, k in events] + [(1, keeps + i) for i in range(parts)]
    place = {slot: s for s, slot in enumerate(slots)}
    orders = []
    for r in range(rings):
        behind = lambda d: r if d > r else rings - 1 - r
        others = [d for d in range(rings) if d != r]
        orders.append(sorted(others, key=lambda d: (-abs(d - r), -behind(d), d)) + [r])
    done = [{} for _ in range(rings)]
    merges = [[0] * len(slots) for _ in range(rings)]
    for s in range(crosses + keeps):
        for r in range(rings):
            k = len(done[r])
            if k == keeps or place[1, k] > s or place[0, k] + 3 > s:
                continue
            d, i = orders[r][k // parts], k % parts
            before = r - 1 if d > r else r + 1
            if 0 <= before < rings and done[before].get((d, i), s) + 3 > s:
                continue
            done[r][d, i] = s
            merges[r][s] = k + 1
    complete = all(len(d) == keeps for d in done)
    return slots, orders, merges, complete


def pick(values, i):
    out = values[-1]
    for k in reversed(range(len(values) - 1)):
        if values[k] != values[k + 1] or not isinstance(out, (int, float)):
            out = jnp.where(i == k, values[k], out)
    return out


def pick_row(rows, r, i):
    out = None
    unique = []
    for row in rows:
        if row not in unique:
            unique.append(row)
    for row in unique:
        mine = pick(row, i)
        if out is None:
            out = mine
        else:
            here = functools.reduce(jnp.logical_or, [r == k for k in range(len(rows)) if rows[k] == row])
            out = jnp.where(here, mine, out)
    return out


def column(row):
    return jnp.transpose(jnp.broadcast_to(row, (LANES, LANES)))


def spread(square, total, share):
    return jnp.maximum(square - total * total * share, square * 1e-5 + 1e-30)


def encode(q):
    size = jnp.clip(jnp.abs(q), 1e-30, 1.04)
    size = jnp.exp2(size * lax.rsqrt(size) * SPAN - BASE)
    return jnp.where(q < 0, -size, size).astype(jnp.bfloat16)


def decode(code):
    y = code.astype(jnp.float32)
    size = jnp.log2(jnp.abs(y)) + BASE
    size = size * size
    return jnp.where(y < 0, -size, size)


def kernel(groups, plan, a_hbm, b_hbm, out, a, g, held, cross_out, cross_in, far_out, far_in,
           sa_own, sa_near, sa_pair, sa_in, sa_run, sa_stat, sb_half, sb_mine, sb_near, sb_run, sb_in,
           a_sem, b_sem, px_send, px_recv, nx_send, nx_recv, fw_send, fw_recv,
           c_send, cb_send, c_recv, f_send, fb_send, f_recv,
           ca_send, ca_recv, fa_send, fa_recv, ready, go):
    slots, orders, merges, _ = plan
    t = lax.axis_index("tok")
    u = lax.axis_index("unit")
    rows, units = b_hbm.shape
    tokens, own = a.shape
    band = units // groups
    parts = band // LANES
    rings = groups // 2
    crosses = rings * parts
    keeps = crosses - parts
    steps = len(slots)
    main = steps - parts
    bunch = steps // BUNCHES
    half = tokens // 2
    r = t // 2
    y = t % 2
    side = u // 2
    partner = u + 1 - 2 * (u % 2)
    across = (u + 2) % 4
    near = t + 1 - 2 * y
    shares = [1.0 / (2 * tokens * max(k, 1)) for k in range(rings + 1)]
    packed = [kind + 2 * (k // parts) + 2048 * (k % parts) for kind, k in slots]

    def slot(s):
        code = pick(packed, s)
        kind, p, i = code % 2, (code // 2) % 1024, code // 2048
        return kind, p, i

    def bound(p):
        return pick_row(orders, r, p)

    def columns(kind, p, i):
        owner = bound(p) * 2 + jnp.where(kind == 0, 1 - y, y)
        return pl.ds(pl.multiple_of(owner * band + i * LANES, LANES), LANES)

    def block(ref, who, cols):
        return ref.at[pl.ds(pl.multiple_of(who * rows, rows), rows), cols]

    def remote(src, dst, send, recv, tt, uu):
        return pltpu.make_async_remote_copy(
            src_ref=src, dst_ref=dst, send_sem=send, recv_sem=recv,
            device_id=(tt, uu), device_id_type=MESH)

    def to_partner(s, cols):
        return remote(b_hbm.at[:, cols], block(g, u, cols), px_send.at[0], px_recv.at[s // bunch], t, partner)

    def to_across(s, cols):
        return remote(block(g, u, cols), block(g, u, cols), nx_send.at[0], nx_recv.at[s % (2 * AHEAD)],
                      t, across)

    def forward(s, cols):
        return remote(block(g, across, cols), block(g, across, cols), fw_send.at[0],
                      fw_recv.at[2 * (s % 2)], t, partner)

    def piece(who, h, cols):
        size = rows // 2
        return g.at[pl.ds(pl.multiple_of(who * rows + h * size, size), size), cols]

    def last_across(i, h, cols):
        return remote(piece(u, h, cols), piece(u, h, cols),
                      nx_send.at[0], nx_recv.at[2 * AHEAD + 2 * i + h], t, across)

    def last_forward(s, h, cols):
        return remote(piece(across, h, cols), piece(across, h, cols), fw_send.at[0],
                      fw_recv.at[2 * (s % 2) + h], t, partner)

    def issue_across(s):
        cols = columns(*slot(s))

        @pl.when(s < main)
        def _():
            to_across(s, cols).start()

        @pl.when(jnp.logical_and(s >= main, s < steps))
        def _():
            for h in (0, 1):
                last_across(s - main, h, cols).start()

    def send_cross(k):
        return remote(cross_out.at[k], cross_in.at[k], c_send.at[0], c_recv.at[k], near, u)

    def send_cross_sums(k):
        return remote(sb_mine.at[k], sb_near.at[k], cb_send.at[0], c_recv.at[k], near, u)

    def both(sem):
        some = g.at[pl.ds(0, own + 16), pl.ds(0, LANES)]
        return pltpu.make_async_copy(some, some, sem)

    def send_far(k, j, tt):
        return remote(far_out.at[k], far_in.at[j], f_send.at[0], f_recv.at[j], tt, u)

    def send_far_sums(k, j, tt):
        return remote(sb_run.at[k], sb_in.at[j], fb_send.at[0], f_recv.at[j], tt, u)

    send_near_a = remote(sa_own, sa_near, ca_send.at[0], ca_recv.at[0], near, u)

    def send_run_a(way):
        tt = t + 2 if way == 0 else t - 2
        return remote(sa_run.at[way], sa_in.at[way], fa_send.at[way], fa_recv.at[way], tt, u)

    a_copy = pltpu.make_async_copy(a_hbm, a, a_sem)
    own_rows = pl.ds(pl.multiple_of(u * rows, rows), rows)

    def b_copy(s):
        cols = columns(*slot(s))
        return pltpu.make_async_copy(
            b_hbm.at[:, cols], g.at[own_rows, cols], b_sem.at[jnp.where(s == 0, 0, jnp.where(s < AHEAD, 1, 2))])

    def b_wait(which, count):
        cols = pl.ds(0, LANES * count)
        pltpu.make_async_copy(b_hbm.at[:, cols], g.at[own_rows, cols], b_sem.at[which]).wait()

    barrier = pltpu.get_barrier_semaphore()

    early_core = u % 2 == 0
    wide_core = u % 2 == 1
    peers = 1 + jnp.where(r > 0, 1, 0) + jnp.where(r < rings - 1, 1, 0)

    def tell(sem, tt, uu):
        pl.semaphore_signal(sem, inc=1, device_id=(tt, uu), device_id_type=MESH)

    def tell_peers(sem):
        tell(sem, near, u)

        @pl.when(r > 0)
        def _():
            tell(sem, t - 2, u)

        @pl.when(r < rings - 1)
        def _():
            tell(sem, t + 2, u)

    tell(barrier, t, across)
    tell(barrier, t, partner)

    @pl.when(wide_core)
    def _():
        tell_peers(barrier)

    @pl.loop(0, AHEAD)
    def _(s):
        b_copy(s).start()

    a_copy.start()
    pl.semaphore_wait(barrier, 2 + jnp.where(wide_core, peers, 0))

    @pl.when(wide_core)
    def _():
        tell_peers(ready)

    b_wait(0, 1)
    issue_across(jnp.int32(0))
    b_wait(1, AHEAD - 1)

    @pl.loop(1, AHEAD)
    def _(s):
        issue_across(s)

    @pl.loop(0, steps)
    def _(s):
        to_partner(s, columns(*slot(s))).start()

        @pl.when(s >= AHEAD)
        def _():
            b_copy(s).start()

    b_wait(2, steps - AHEAD)
    a_copy.wait()
    chunk = 128

    def sum_rows(wide):
        wide = wide.astype(jnp.float32).reshape(wide.shape[0] // 8, 8, wide.shape[1])
        return jnp.sum(wide, axis=0), jnp.sum(wide * wide, axis=0)

    def body(i, carry):
        total, square = sum_rows(a[pl.ds(pl.multiple_of(i * chunk, chunk), chunk), :])
        return carry[0] + total, carry[1] + square

    zero = jnp.zeros((8, own), jnp.float32)
    total, square = lax.fori_loop(0, tokens // chunk, body, (zero, zero))
    sa_own[...] = jnp.zeros((8, own), jnp.float32)
    sa_own[0:1, :] = jnp.sum(total, axis=0, keepdims=True)
    sa_own[1:2, :] = jnp.sum(square, axis=0, keepdims=True)

    @pl.when(wide_core)
    def _():
        pl.semaphore_wait(ready, peers)
        tell(go, t, partner)

    @pl.when(early_core)
    def _():
        pl.semaphore_wait(go, 1)

    send_near_a.start()

    def tiles():
        return [slice(c * LANES, (c + 1) * LANES) for c in range(own // LANES)]

    def early(hold, cols):
        mine = pl.ds(pl.multiple_of(side * half, half), half)
        lhs = g[mine, cols]
        held[hold] = contract_tokens(lhs, a[mine, :])
        total, square = sum_rows(lhs)
        sb_half[0] = total
        sb_half[1] = square

    def part(hold, start, size, cols):
        some = pl.ds(pl.multiple_of(start, size), size)
        lhs = g[some, cols]
        held[hold] = held[hold] + contract_tokens(lhs, a[some, :])
        total, square = sum_rows(lhs)
        sb_half[0] = sb_half[0] + total
        sb_half[1] = sb_half[1] + square

    def finish_sums(k):
        sb_mine[k] = jnp.zeros((8, LANES), jnp.float32)
        sb_mine[k, 0:1, :] = jnp.sum(sb_half[0], axis=0, keepdims=True)
        sb_mine[k, 1:2, :] = jnp.sum(sb_half[1], axis=0, keepdims=True)

    def put(target, k, hold, sb, sa, share):
        tb, qb = sb[0:1, :], sb[1:2, :]
        tb_col = column(tb * share)
        scale_col = column(lax.rsqrt(spread(qb, tb, share)))
        for cols in tiles():
            ta = sa[0:1, cols]
            scale = lax.rsqrt(spread(sa[1:2, cols], ta, share))
            q = (held[hold, :, cols] - tb_col * ta) * (scale_col * scale)
            target[k, :, cols] = encode(q)

    def take(hold, source, k, sb, sa, share):
        tb, qb = sb[0:1, :], sb[1:2, :]
        tb_col = column(tb * share)
        norm_col = column(jnp.sqrt(spread(qb, tb, share)) * (1.0 / (SPAN * SPAN)))
        for cols in tiles():
            ta = sa[0:1, cols]
            norm = jnp.sqrt(spread(sa[1:2, cols], ta, share))
            held[hold, :, cols] = held[hold, :, cols] + (
                decode(source[k, :, cols]) * (norm_col * norm) + tb_col * ta)

    def take_near(k):
        both(c_recv.at[k]).wait()
        take(k, cross_in, k, sb_near.at[k], sa_near, 1.0 / tokens)

    def take_far(way, k, j):
        both(f_recv.at[j]).wait()
        count = jnp.where(way == 0, r, rings - 1 - r)
        take(k, far_in, j, sb_in.at[j], sa_in.at[way], pick(shares, count))

    def route(k):
        p, i = k // parts, k % parts
        d = bound(p)
        way = jnp.where(d > r, 0, 1)
        count = jnp.where(way == 0, r, rings - 1 - r)
        distance = jnp.where(way == 0, d - r, r - d)
        return way, count, (way * (rings - 1) + distance) * parts + i

    def collect(k):
        way, count, j = route(k)
        take_near(k)

        @pl.when(count > 0)
        def _():
            take_far(way, k, j)

    def pass_on(k):
        way, count, j = route(k)
        sb_run[k] = sb_mine[crosses + k] + sb_near[k]

        @pl.when(count > 0)
        def _():
            sb_run[k] = sb_run[k] + sb_in[j]

        put(far_out, k, k, sb_run.at[k], sa_run.at[way], pick(shares, count + 1))
        tt = t + 2 - 4 * way
        send_far(k, j - parts, tt).start()
        send_far_sums(k, j - parts, tt).start()

    def exchange_a(s):
        @pl.when(s == 1)
        def _():
            send_near_a.wait_recv()
            sa_pair[...] = sa_own[...] + sa_near[...]

        for way, ready in ((0, r + 1), (1, rings - r)):
            first = (r == 0) if way == 0 else (r == rings - 1)
            final = (r == rings - 1) if way == 0 else (r == 0)

            @pl.when(jnp.logical_and(s == ready, first))
            def _():
                sa_in[way] = jnp.zeros((8, own), jnp.float32)
                sa_run[way] = sa_pair[...]

            @pl.when(jnp.logical_and(s == ready, jnp.logical_not(first)))
            def _():
                send_run_a(way).wait_recv()
                sa_run[way] = sa_pair[...] + sa_in[way]

            @pl.when(jnp.logical_and(s == ready, jnp.logical_not(final)))
            def _():
                send_run_a(way).start()

    def partner_ready(s):
        @pl.when(s % bunch == 0)
        def _():
            to_partner(s, pl.ds(0, LANES * bunch)).wait_recv()

    @pl.loop(0, main)
    def _(s):
        kind, p, i = slot(s)
        cols = columns(kind, p, i)
        k = p * parts + i
        hold = jnp.where(kind == 0, crosses, k)
        partner_ready(s)
        early(hold, cols)
        to_across(s, cols).wait_recv()
        forward(s, cols).start()
        issue_across(s + AHEAD)
        exchange_a(s)
        pair = pick_row(merges, r, s)

        @pl.when(pair > 0)
        def _():
            collect(pair - 1)

        part(hold, across * rows, rows, cols)
        forward(s, cols).wait_recv()
        part(hold, (across + 1 - 2 * (across % 2)) * rows, rows, cols)
        finish_sums(kind * crosses + k)

        @pl.when(kind == 0)
        def _():
            put(cross_out, k, hold, sb_mine.at[k], sa_own, 1.0 / tokens)
            send_cross(k).start()
            send_cross_sums(k).start()

        @pl.when(pair > 0)
        def _():
            pass_on(pair - 1)

    whole_a = sa_pair[...] + sa_in[0] + sa_in[1]
    total_tokens = tokens * groups
    mean_a = whole_a[0:1, :] * (1.0 / total_tokens)
    var_a = whole_a[1:2, :] * (1.0 / total_tokens) - mean_a * mean_a
    sa_stat[0:1, :] = mean_a
    sa_stat[1:2, :] = 1.0 / jnp.sqrt(var_a + 1e-05)

    @pl.loop(0, parts)
    def _(i):
        s = main + i
        k = keeps + i
        cols = pl.ds(pl.multiple_of(t * band + i * LANES, LANES), LANES)
        partner_ready(s)
        early(k, cols)
        for h in (0, 1):
            last_across(i, h, cols).wait_recv()
            last_forward(s, h, cols).start()
        part(k, across * rows, rows, cols)
        take_near(k)
        sb_half[2] = sb_near[k]
        for way, some in ((0, r > 0), (1, r < rings - 1)):
            @pl.when(some)
            def _():
                j = way * (rings - 1) * parts + i
                take_far(way, k, j)
                sb_half[2] = sb_half[2] + sb_in[j]

        for h in (0, 1):
            last_forward(s, h, cols).wait_recv()
            part(k, (across + 1 - 2 * (across % 2)) * rows + h * (rows // 2), rows // 2, cols)
        finish_sums(crosses + k)
        whole_b = sb_half[2] + sb_mine[crosses + k]
        mean_b = whole_b[0:1, :] * (1.0 / total_tokens)
        var_b = whole_b[1:2, :] * (1.0 / total_tokens) - mean_b * mean_b
        mean_col = column(mean_b)
        inv_col = column(1.0 / jnp.sqrt(var_b + 1e-05))
        lanes = pl.ds(pl.multiple_of(i * LANES, LANES), LANES)
        for c in tiles():
            centered = held[k, :, c] * (1.0 / total_tokens) - mean_col * sa_stat[0:1, c]
            out[lanes, c] = centered * (inv_col * sa_stat[1:2, c])

    send_near_a.wait_send()

    @pl.when(r < rings - 1)
    def _():
        send_run_a(0).wait_send()

    @pl.when(r > 0)
    def _():
        send_run_a(1).wait_send()

    own_b = g.at[own_rows, :]
    remote(own_b, own_b, nx_send.at[0], nx_recv.at[0], t, across).wait_send()
    remote(b_hbm, own_b, px_send.at[0], px_recv.at[0], t, partner).wait_send()
    remote(own_b, own_b, fw_send.at[0], fw_recv.at[0], t, partner).wait_send()
    remote(cross_out, cross_in, c_send.at[0], c_recv.at[0], near, u).wait_send()
    remote(sb_near, sb_near, cb_send.at[0], c_recv.at[0], near, u).wait_send()
    remote(far_out, far_out, f_send.at[0], f_recv.at[0], near, u).wait_send()
    remote(sb_run, sb_run, fb_send.at[0], f_recv.at[0], near, u).wait_send()


def fused(groups, plan, act_a, act_b):
    tokens, own = act_a.shape
    rows, units = act_b.shape
    band = units // groups
    parts = band // LANES
    rings = groups // 2
    crosses = rings * parts
    keeps = crosses - parts
    steps = 2 * crosses
    dma = lambda n: pltpu.SemaphoreType.DMA((n,))
    bf16 = lambda *shape: pltpu.VMEM(shape, jnp.bfloat16)
    f32 = lambda *shape: pltpu.VMEM(shape, jnp.float32)
    return pl.pallas_call(
        functools.partial(kernel, groups, plan),
        out_shape=jax.ShapeDtypeStruct((band, own), jnp.float32),
        in_specs=[pl.BlockSpec(memory_space=pltpu.HBM)] * 2,
        out_specs=pl.BlockSpec(memory_space=pltpu.VMEM),
        scratch_shapes=[
            bf16(tokens, own),
            bf16(tokens, units),
            f32(crosses + 1, LANES, own),
            bf16(crosses, LANES, own),
            bf16(crosses, LANES, own),
            bf16(keeps, LANES, own),
            bf16(2 * keeps, LANES, own),
            f32(8, own), f32(8, own), f32(8, own),
            f32(2, 8, own), f32(2, 8, own), f32(8, own),
            f32(3, 8, LANES),
            f32(2 * crosses, 8, LANES), f32(crosses, 8, LANES),
            f32(keeps, 8, LANES), f32(2 * keeps, 8, LANES),
            pltpu.SemaphoreType.DMA, dma(3),
            dma(1), dma(BUNCHES),
            dma(1), dma(2 * AHEAD + 2 * parts),
            dma(1), dma(4),
            dma(1), dma(1), dma(crosses),
            dma(1), dma(1), dma(2 * keeps),
            dma(1), dma(1),
            dma(2), dma(2),
            pltpu.SemaphoreType.REGULAR, pltpu.SemaphoreType.REGULAR,
        ],
        compiler_params=pltpu.CompilerParams(
            collective_id=0, has_side_effects=True, vmem_limit_bytes=52000 * 1024
        ),
        name="gather_correlate",
    )(act_a, act_b)


def solution(mesh):
    groups, split = mesh.shape["tok"], mesh.shape["unit"]

    def per_device(act_a, act_b):
        band = act_b.shape[1] // groups
        whole = act_a.shape[0] % 256 == 0 and act_a.shape[1] % LANES == 0
        if split == 4 and groups % 2 == 0 and groups > 4 and band % LANES == 0 and whole:
            plan = schedule(groups // 2, band // LANES)
            if plan[-1] and len(plan[0]) % BUNCHES == 0:
                return fused(groups, plan, act_a, act_b)
        return plain(act_a, act_b)

    placed = (P("tok", "unit"), P(("tok", "unit"), None))
    return jax.shard_map(
        per_device, mesh=mesh, in_specs=placed, out_specs=P("tok", "unit"), check_vma=False
    )
```

```python
import functools

import jax
import jax.numpy as jnp
from jax import lax
from jax.experimental import pallas as pl
from jax.experimental.pallas import tpu as pltpu
from jax.sharding import PartitionSpec as P

MESH = pl.DeviceIdType.MESH
LANES = 128
SPAN = 244.0
BASE = 122.0
AHEAD = 4
BUNCHES = 4


def contract_tokens(left, right):
    return lax.dot_general(
        left, right, (((0,), (0,)), ((), ())), preferred_element_type=jnp.float32
    )


def plain(act_a, act_b):
    token_rows = act_a.shape[0]
    units = act_b.shape[1]
    groups = lax.axis_size("tok")
    band = units // groups
    total_tokens = token_rows * groups
    wide_a = act_a.astype(jnp.float32)
    first_total = jnp.sum(wide_a, axis=0)
    first_square = jnp.sum(wide_a * wide_a, axis=0)
    piece = lax.all_gather(act_b, "unit", axis=0, tiled=True)
    product = contract_tokens(piece, act_a)
    wide_piece = piece.astype(jnp.float32)
    second_total = jnp.sum(wide_piece, axis=0)
    second_square = jnp.sum(wide_piece * wide_piece, axis=0)
    shares = lax.psum_scatter(product, "tok", scatter_dimension=0, tiled=True)
    first_all, first_square_all, second_all, second_square_all = lax.psum(
        (first_total, first_square, second_total, second_square), "tok"
    )
    offset = lax.axis_index("tok") * band
    second_own = lax.dynamic_slice_in_dim(second_all, offset, band, 0)
    second_square_own = lax.dynamic_slice_in_dim(second_square_all, offset, band, 0)
    mean_a = first_all / total_tokens
    var_a = first_square_all / total_tokens - mean_a * mean_a
    mean_b = second_own / total_tokens
    var_b = second_square_own / total_tokens - mean_b * mean_b
    centered = shares / total_tokens - mean_b[:, None] * mean_a[None, :]
    return centered / (jnp.sqrt(var_b + 1e-05)[:, None] * jnp.sqrt(var_a + 1e-05)[None, :])


def schedule(rings, parts):
    crosses, keeps = rings * parts, (rings - 1) * parts
    events = sorted(
        [((k + 0.25) / crosses, 0, k) for k in range(crosses)]
        + [((k + 1) / keeps, 1, k) for k in range(keeps)]
    )
    slots = [(kind, k) for _, kind, k in events] + [(1, keeps + i) for i in range(parts)]
    place = {slot: s for s, slot in enumerate(slots)}
    orders = []
    for r in range(rings):
        behind = lambda d: r if d > r else rings - 1 - r
        others = [d for d in range(rings) if d != r]
        orders.append(sorted(others, key=lambda d: (-abs(d - r), -behind(d), d)) + [r])
    done = [{} for _ in range(rings)]
    merges = [[0] * len(slots) for _ in range(rings)]
    for s in range(crosses + keeps):
        for r in range(rings):
            k = len(done[r])
            if k == keeps or place[1, k] > s or place[0, k] + 3 > s:
                continue
            d, i = orders[r][k // parts], k % parts
            before = r - 1 if d > r else r + 1
            if 0 <= before < rings and done[before].get((d, i), s) + 3 > s:
                continue
            done[r][d, i] = s
            merges[r][s] = k + 1
    complete = all(len(d) == keeps for d in done)
    return slots, orders, merges, complete


def pick(values, i):
    out = values[-1]
    for k in reversed(range(len(values) - 1)):
        if values[k] != values[k + 1] or not isinstance(out, (int, float)):
            out = jnp.where(i == k, values[k], out)
    return out


def pick_row(rows, r, i):
    out = None
    unique = []
    for row in rows:
        if row not in unique:
            unique.append(row)
    for row in unique:
        mine = pick(row, i)
        if out is None:
            out = mine
        else:
            here = functools.reduce(jnp.logical_or, [r == k for k in range(len(rows)) if rows[k] == row])
            out = jnp.where(here, mine, out)
    return out


def column(row):
    return jnp.transpose(jnp.broadcast_to(row, (LANES, LANES)))


def spread(square, total, share):
    return jnp.maximum(square - total * total * share, square * 1e-5 + 1e-30)


def encode(q):
    size = jnp.clip(jnp.abs(q), 1e-30, 1.04)
    size = jnp.exp2(size * lax.rsqrt(size) * SPAN - BASE)
    return jnp.where(q < 0, -size, size).astype(jnp.bfloat16)


def decode(code):
    y = code.astype(jnp.float32)
    size = jnp.log2(jnp.abs(y)) + BASE
    size = size * size
    return jnp.where(y < 0, -size, size)


def work(groups, plan, a_hbm, b_hbm, out, a, g, held, cross_out, cross_in, far_out, far_in,
           sa_own, sa_near, sa_pair, sa_in, sa_run, sa_stat, sb_half, sb_mine, sb_near, sb_run, sb_in,
           a_sem, b_sem, px_send, px_recv, nx_send, nx_recv, fw_send, fw_recv,
           c_send, cb_send, c_recv, f_send, fb_send, f_recv,
           ca_send, ca_recv, fa_send, fa_recv, ready, go):
    slots, orders, merges, _ = plan
    t = lax.axis_index("tok")
    u = lax.axis_index("unit")
    rows, units = b_hbm.shape
    tokens, own = a.shape
    band = units // groups
    parts = band // LANES
    rings = groups // 2
    crosses = rings * parts
    keeps = crosses - parts
    steps = len(slots)
    main = steps - parts
    bunch = steps // BUNCHES
    half = tokens // 2
    r = t // 2
    y = t % 2
    side = u // 2
    partner = u + 1 - 2 * (u % 2)
    across = (u + 2) % 4
    near = t + 1 - 2 * y
    shares = [1.0 / (2 * tokens * max(k, 1)) for k in range(rings + 1)]
    packed = [kind + 2 * (k // parts) + 2048 * (k % parts) for kind, k in slots]

    def slot(s):
        code = pick(packed, s)
        kind, p, i = code % 2, (code // 2) % 1024, code // 2048
        return kind, p, i

    def bound(p):
        return pick_row(orders, r, p)

    def columns(kind, p, i):
        owner = bound(p) * 2 + jnp.where(kind == 0, 1 - y, y)
        return pl.ds(pl.multiple_of(owner * band + i * LANES, LANES), LANES)

    def block(ref, who, cols):
        return ref.at[pl.ds(pl.multiple_of(who * rows, rows), rows), cols]

    def remote(src, dst, send, recv, tt, uu):
        return pltpu.make_async_remote_copy(
            src_ref=src, dst_ref=dst, send_sem=send, recv_sem=recv,
            device_id=(tt, uu), device_id_type=MESH)

    def to_partner(s, cols):
        return remote(b_hbm.at[:, cols], block(g, u, cols), px_send.at[0], px_recv.at[s // bunch], t, partner)

    def to_across(s, cols):
        return remote(block(g, u, cols), block(g, u, cols), nx_send.at[0], nx_recv.at[s % (2 * AHEAD)],
                      t, across)

    def forward(s, cols):
        return remote(block(g, across, cols), block(g, across, cols), fw_send.at[0],
                      fw_recv.at[2 * (s % 2)], t, partner)

    def piece(who, h, cols):
        size = rows // 2
        return g.at[pl.ds(pl.multiple_of(who * rows + h * size, size), size), cols]

    def last_across(i, h, cols):
        return remote(piece(u, h, cols), piece(u, h, cols),
                      nx_send.at[0], nx_recv.at[2 * AHEAD + 2 * i + h], t, across)

    def last_forward(s, h, cols):
        return remote(piece(across, h, cols), piece(across, h, cols), fw_send.at[0],
                      fw_recv.at[2 * (s % 2) + h], t, partner)

    def issue_across(s):
        cols = columns(*slot(s))

        @pl.when(s < main)
        def _():
            to_across(s, cols).start()

        @pl.when(jnp.logical_and(s >= main, s < steps))
        def _():
            for h in (0, 1):
                last_across(s - main, h, cols).start()

    def send_cross(k):
        return remote(cross_out.at[k], cross_in.at[k], c_send.at[0], c_recv.at[k], near, u)

    def send_cross_sums(k):
        return remote(sb_mine.at[k], sb_near.at[k], cb_send.at[0], c_recv.at[k], near, u)

    def both(sem):
        some = g.at[pl.ds(0, own + 16), pl.ds(0, LANES)]
        return pltpu.make_async_copy(some, some, sem)

    def send_far(k, j, tt):
        return remote(far_out.at[k], far_in.at[j], f_send.at[0], f_recv.at[j], tt, u)

    def send_far_sums(k, j, tt):
        return remote(sb_run.at[k], sb_in.at[j], fb_send.at[0], f_recv.at[j], tt, u)

    send_near_a = remote(sa_own, sa_near, ca_send.at[0], ca_recv.at[0], near, u)

    def send_run_a(way):
        tt = t + 2 if way == 0 else t - 2
        return remote(sa_run.at[way], sa_in.at[way], fa_send.at[way], fa_recv.at[way], tt, u)

    a_copy = pltpu.make_async_copy(a_hbm, a, a_sem)
    own_rows = pl.ds(pl.multiple_of(u * rows, rows), rows)

    def b_copy(s):
        cols = columns(*slot(s))
        return pltpu.make_async_copy(
            b_hbm.at[:, cols], g.at[own_rows, cols], b_sem.at[jnp.where(s == 0, 0, jnp.where(s < AHEAD, 1, 2))])

    def b_wait(which, count):
        cols = pl.ds(0, LANES * count)
        pltpu.make_async_copy(b_hbm.at[:, cols], g.at[own_rows, cols], b_sem.at[which]).wait()

    barrier = pltpu.get_barrier_semaphore()

    early_core = u % 2 == 0
    wide_core = u % 2 == 1
    peers = 1 + jnp.where(r > 0, 1, 0) + jnp.where(r < rings - 1, 1, 0)

    def tell(sem, tt, uu):
        pl.semaphore_signal(sem, inc=1, device_id=(tt, uu), device_id_type=MESH)

    def tell_peers(sem):
        tell(sem, near, u)

        @pl.when(r > 0)
        def _():
            tell(sem, t - 2, u)

        @pl.when(r < rings - 1)
        def _():
            tell(sem, t + 2, u)

    tell(barrier, t, across)
    tell(barrier, t, partner)

    @pl.when(wide_core)
    def _():
        tell_peers(barrier)

    @pl.loop(0, AHEAD)
    def _(s):
        b_copy(s).start()

    a_copy.start()
    pl.semaphore_wait(barrier, 2 + jnp.where(wide_core, peers, 0))

    @pl.when(wide_core)
    def _():
        tell_peers(ready)

    b_wait(0, 1)
    issue_across(jnp.int32(0))
    b_wait(1, AHEAD - 1)

    @pl.loop(1, AHEAD)
    def _(s):
        issue_across(s)

    @pl.loop(0, steps)
    def _(s):
        to_partner(s, columns(*slot(s))).start()

        @pl.when(s >= AHEAD)
        def _():
            b_copy(s).start()

    b_wait(2, steps - AHEAD)
    a_copy.wait()
    chunk = 128

    def sum_rows(wide):
        wide = wide.astype(jnp.float32).reshape(wide.shape[0] // 8, 8, wide.shape[1])
        return jnp.sum(wide, axis=0), jnp.sum(wide * wide, axis=0)

    def body(i, carry):
        total, square = sum_rows(a[pl.ds(pl.multiple_of(i * chunk, chunk), chunk), :])
        return carry[0] + total, carry[1] + square

    zero = jnp.zeros((8, own), jnp.float32)
    total, square = lax.fori_loop(0, tokens // chunk, body, (zero, zero))
    sa_own[...] = jnp.zeros((8, own), jnp.float32)
    sa_own[0:1, :] = jnp.sum(total, axis=0, keepdims=True)
    sa_own[1:2, :] = jnp.sum(square, axis=0, keepdims=True)

    @pl.when(wide_core)
    def _():
        pl.semaphore_wait(ready, peers)
        tell(go, t, partner)

    @pl.when(early_core)
    def _():
        pl.semaphore_wait(go, 1)

    send_near_a.start()

    def tiles():
        return [slice(c * LANES, (c + 1) * LANES) for c in range(own // LANES)]

    def early(hold, cols):
        mine = pl.ds(pl.multiple_of(side * half, half), half)
        lhs = g[mine, cols]
        held[hold] = contract_tokens(lhs, a[mine, :])
        total, square = sum_rows(lhs)
        sb_half[0] = total
        sb_half[1] = square

    def part(hold, start, size, cols):
        some = pl.ds(pl.multiple_of(start, size), size)
        lhs = g[some, cols]
        held[hold] = held[hold] + contract_tokens(lhs, a[some, :])
        total, square = sum_rows(lhs)
        sb_half[0] = sb_half[0] + total
        sb_half[1] = sb_half[1] + square

    def finish_sums(k):
        sb_mine[k] = jnp.zeros((8, LANES), jnp.float32)
        sb_mine[k, 0:1, :] = jnp.sum(sb_half[0], axis=0, keepdims=True)
        sb_mine[k, 1:2, :] = jnp.sum(sb_half[1], axis=0, keepdims=True)

    def put(target, k, hold, sb, sa, share):
        tb, qb = sb[0:1, :], sb[1:2, :]
        tb_col = column(tb * share)
        scale_col = column(lax.rsqrt(spread(qb, tb, share)))
        for cols in tiles():
            ta = sa[0:1, cols]
            scale = lax.rsqrt(spread(sa[1:2, cols], ta, share))
            q = (held[hold, :, cols] - tb_col * ta) * (scale_col * scale)
            target[k, :, cols] = encode(q)

    def take(hold, source, k, sb, sa, share):
        tb, qb = sb[0:1, :], sb[1:2, :]
        tb_col = column(tb * share)
        norm_col = column(jnp.sqrt(spread(qb, tb, share)) * (1.0 / (SPAN * SPAN)))
        for cols in tiles():
            ta = sa[0:1, cols]
            norm = jnp.sqrt(spread(sa[1:2, cols], ta, share))
            held[hold, :, cols] = held[hold, :, cols] + (
                decode(source[k, :, cols]) * (norm_col * norm) + tb_col * ta)

    def take_near(k):
        both(c_recv.at[k]).wait()
        take(k, cross_in, k, sb_near.at[k], sa_near, 1.0 / tokens)

    def take_far(way, k, j):
        both(f_recv.at[j]).wait()
        count = jnp.where(way == 0, r, rings - 1 - r)
        take(k, far_in, j, sb_in.at[j], sa_in.at[way], pick(shares, count))

    def route(k):
        p, i = k // parts, k % parts
        d = bound(p)
        way = jnp.where(d > r, 0, 1)
        count = jnp.where(way == 0, r, rings - 1 - r)
        distance = jnp.where(way == 0, d - r, r - d)
        return way, count, (way * (rings - 1) + distance) * parts + i

    def collect(k):
        way, count, j = route(k)
        take_near(k)

        @pl.when(count > 0)
        def _():
            take_far(way, k, j)

    def pass_on(k):
        way, count, j = route(k)
        sb_run[k] = sb_mine[crosses + k] + sb_near[k]

        @pl.when(count > 0)
        def _():
            sb_run[k] = sb_run[k] + sb_in[j]

        put(far_out, k, k, sb_run.at[k], sa_run.at[way], pick(shares, count + 1))
        tt = t + 2 - 4 * way
        send_far(k, j - parts, tt).start()
        send_far_sums(k, j - parts, tt).start()

    def exchange_a(s):
        @pl.when(s == 1)
        def _():
            send_near_a.wait_recv()
            sa_pair[...] = sa_own[...] + sa_near[...]

        for way, ready in ((0, r + 1), (1, rings - r)):
            first = (r == 0) if way == 0 else (r == rings - 1)
            final = (r == rings - 1) if way == 0 else (r == 0)

            @pl.when(jnp.logical_and(s == ready, first))
            def _():
                sa_in[way] = jnp.zeros((8, own), jnp.float32)
                sa_run[way] = sa_pair[...]

            @pl.when(jnp.logical_and(s == ready, jnp.logical_not(first)))
            def _():
                send_run_a(way).wait_recv()
                sa_run[way] = sa_pair[...] + sa_in[way]

            @pl.when(jnp.logical_and(s == ready, jnp.logical_not(final)))
            def _():
                send_run_a(way).start()

    def partner_ready(s):
        @pl.when(s % bunch == 0)
        def _():
            to_partner(s, pl.ds(0, LANES * bunch)).wait_recv()

    @pl.loop(0, main)
    def _(s):
        kind, p, i = slot(s)
        cols = columns(kind, p, i)
        k = p * parts + i
        hold = jnp.where(kind == 0, crosses, k)
        partner_ready(s)
        early(hold, cols)
        to_across(s, cols).wait_recv()
        forward(s, cols).start()
        issue_across(s + AHEAD)
        exchange_a(s)
        pair = pick_row(merges, r, s)

        @pl.when(pair > 0)
        def _():
            collect(pair - 1)

        part(hold, across * rows, rows, cols)
        forward(s, cols).wait_recv()
        part(hold, (across + 1 - 2 * (across % 2)) * rows, rows, cols)
        finish_sums(kind * crosses + k)

        @pl.when(kind == 0)
        def _():
            put(cross_out, k, hold, sb_mine.at[k], sa_own, 1.0 / tokens)
            send_cross(k).start()
            send_cross_sums(k).start()

        @pl.when(pair > 0)
        def _():
            pass_on(pair - 1)

    whole_a = sa_pair[...] + sa_in[0] + sa_in[1]
    total_tokens = tokens * groups
    mean_a = whole_a[0:1, :] * (1.0 / total_tokens)
    var_a = whole_a[1:2, :] * (1.0 / total_tokens) - mean_a * mean_a
    sa_stat[0:1, :] = mean_a
    sa_stat[1:2, :] = 1.0 / jnp.sqrt(var_a + 1e-05)

    @pl.loop(0, parts)
    def _(i):
        s = main + i
        k = keeps + i
        cols = pl.ds(pl.multiple_of(t * band + i * LANES, LANES), LANES)
        partner_ready(s)
        early(k, cols)
        take_near(k)
        sb_half[2] = sb_near[k]
        for h in (0, 1):
            last_across(i, h, cols).wait_recv()
            last_forward(s, h, cols).start()
            part(k, across * rows + h * (rows // 2), rows // 2, cols)
        for way, some in ((0, r > 0), (1, r < rings - 1)):
            @pl.when(some)
            def _():
                j = way * (rings - 1) * parts + i
                take_far(way, k, j)
                sb_half[2] = sb_half[2] + sb_in[j]

        for h in (0, 1):
            last_forward(s, h, cols).wait_recv()
            part(k, (across + 1 - 2 * (across % 2)) * rows + h * (rows // 2), rows // 2, cols)
        finish_sums(crosses + k)
        whole_b = sb_half[2] + sb_mine[crosses + k]
        mean_b = whole_b[0:1, :] * (1.0 / total_tokens)
        var_b = whole_b[1:2, :] * (1.0 / total_tokens) - mean_b * mean_b
        mean_col = column(mean_b)
        inv_col = column(1.0 / jnp.sqrt(var_b + 1e-05))
        lanes = pl.ds(pl.multiple_of(i * LANES, LANES), LANES)
        for c in tiles():
            centered = held[k, :, c] * (1.0 / total_tokens) - mean_col * sa_stat[0:1, c]
            out[lanes, c] = centered * (inv_col * sa_stat[1:2, c])

    send_near_a.wait_send()

    @pl.when(r < rings - 1)
    def _():
        send_run_a(0).wait_send()

    @pl.when(r > 0)
    def _():
        send_run_a(1).wait_send()

    own_b = g.at[own_rows, :]
    remote(own_b, own_b, nx_send.at[0], nx_recv.at[0], t, across).wait_send()
    remote(b_hbm, own_b, px_send.at[0], px_recv.at[0], t, partner).wait_send()
    remote(own_b, own_b, fw_send.at[0], fw_recv.at[0], t, partner).wait_send()
    remote(cross_out, cross_in, c_send.at[0], c_recv.at[0], near, u).wait_send()
    remote(sb_near, sb_near, cb_send.at[0], c_recv.at[0], near, u).wait_send()
    remote(far_out, far_out, f_send.at[0], f_recv.at[0], near, u).wait_send()
    remote(sb_run, sb_run, fb_send.at[0], f_recv.at[0], near, u).wait_send()


def kernel(groups, plan, semaphores, *refs):
    pl.run_scoped(lambda *sems: work(groups, plan, *refs, *sems), *semaphores)


def fused(groups, plan, act_a, act_b):
    tokens, own = act_a.shape
    rows, units = act_b.shape
    band = units // groups
    parts = band // LANES
    rings = groups // 2
    crosses = rings * parts
    keeps = crosses - parts
    steps = 2 * crosses
    dma = lambda n: pltpu.SemaphoreType.DMA((n,))
    bf16 = lambda *shape: pltpu.VMEM(shape, jnp.bfloat16)
    f32 = lambda *shape: pltpu.VMEM(shape, jnp.float32)
    semaphores = [
        pltpu.SemaphoreType.DMA, dma(3),
        dma(1), dma(BUNCHES),
        dma(1), dma(2 * AHEAD + 2 * parts),
        dma(1), dma(4),
        dma(1), dma(1), dma(crosses),
        dma(1), dma(1), dma(2 * keeps),
        dma(1), dma(1),
        dma(2), dma(2),
        pltpu.SemaphoreType.REGULAR, pltpu.SemaphoreType.REGULAR,
    ]
    return pl.pallas_call(
        functools.partial(kernel, groups, plan, semaphores),
        out_shape=jax.ShapeDtypeStruct((band, own), jnp.float32),
        in_specs=[pl.BlockSpec(memory_space=pltpu.HBM)] * 2,
        out_specs=pl.BlockSpec(memory_space=pltpu.VMEM),
        scratch_shapes=[
            bf16(tokens, own),
            bf16(tokens, units),
            f32(crosses + 1, LANES, own),
            bf16(crosses, LANES, own),
            bf16(crosses, LANES, own),
            bf16(keeps, LANES, own),
            bf16(2 * keeps, LANES, own),
            f32(8, own), f32(8, own), f32(8, own),
            f32(2, 8, own), f32(2, 8, own), f32(8, own),
            f32(3, 8, LANES),
            f32(2 * crosses, 8, LANES), f32(crosses, 8, LANES),
            f32(keeps, 8, LANES), f32(2 * keeps, 8, LANES),
        ],
        compiler_params=pltpu.CompilerParams(
            collective_id=0, has_side_effects=True, vmem_limit_bytes=52000 * 1024
        ),
        name="gather_correlate",
    )(act_a, act_b)


def solution(mesh):
    groups, split = mesh.shape["tok"], mesh.shape["unit"]

    def per_device(act_a, act_b):
        band = act_b.shape[1] // groups
        whole = act_a.shape[0] % 256 == 0 and act_a.shape[1] % LANES == 0
        if split == 4 and groups % 2 == 0 and groups > 4 and band % LANES == 0 and whole:
            plan = schedule(groups // 2, band // LANES)
            if plan[-1] and len(plan[0]) % BUNCHES == 0:
                return fused(groups, plan, act_a, act_b)
        return plain(act_a, act_b)

    placed = (P("tok", "unit"), P(("tok", "unit"), None))
    return jax.shard_map(
        per_device, mesh=mesh, in_specs=placed, out_specs=P("tok", "unit"), check_vma=False
    )
```

```python
import functools

import jax
import jax.numpy as jnp
from jax import lax
from jax.experimental import pallas as pl
from jax.experimental.pallas import tpu as pltpu
from jax.sharding import PartitionSpec as P

MESH = pl.DeviceIdType.MESH
LANES = 128
SPAN = 244.0
BASE = 122.0
AHEAD = 4
BUNCHES = 4


def contract_tokens(left, right):
    return lax.dot_general(
        left, right, (((0,), (0,)), ((), ())), preferred_element_type=jnp.float32
    )


def plain(act_a, act_b):
    token_rows = act_a.shape[0]
    units = act_b.shape[1]
    groups = lax.axis_size("tok")
    band = units // groups
    total_tokens = token_rows * groups
    wide_a = act_a.astype(jnp.float32)
    first_total = jnp.sum(wide_a, axis=0)
    first_square = jnp.sum(wide_a * wide_a, axis=0)
    piece = lax.all_gather(act_b, "unit", axis=0, tiled=True)
    product = contract_tokens(piece, act_a)
    wide_piece = piece.astype(jnp.float32)
    second_total = jnp.sum(wide_piece, axis=0)
    second_square = jnp.sum(wide_piece * wide_piece, axis=0)
    shares = lax.psum_scatter(product, "tok", scatter_dimension=0, tiled=True)
    first_all, first_square_all, second_all, second_square_all = lax.psum(
        (first_total, first_square, second_total, second_square), "tok"
    )
    offset = lax.axis_index("tok") * band
    second_own = lax.dynamic_slice_in_dim(second_all, offset, band, 0)
    second_square_own = lax.dynamic_slice_in_dim(second_square_all, offset, band, 0)
    mean_a = first_all / total_tokens
    var_a = first_square_all / total_tokens - mean_a * mean_a
    mean_b = second_own / total_tokens
    var_b = second_square_own / total_tokens - mean_b * mean_b
    centered = shares / total_tokens - mean_b[:, None] * mean_a[None, :]
    return centered / (jnp.sqrt(var_b + 1e-05)[:, None] * jnp.sqrt(var_a + 1e-05)[None, :])


def schedule(rings, parts):
    crosses, keeps = rings * parts, (rings - 1) * parts
    events = sorted(
        [((k + 0.25) / crosses, 0, k) for k in range(crosses)]
        + [((k + 1) / keeps, 1, k) for k in range(keeps)]
    )
    slots = [(kind, k) for _, kind, k in events] + [(1, keeps + i) for i in range(parts)]
    place = {slot: s for s, slot in enumerate(slots)}
    orders = []
    for r in range(rings):
        behind = lambda d: r if d > r else rings - 1 - r
        others = [d for d in range(rings) if d != r]
        orders.append(sorted(others, key=lambda d: (-abs(d - r), -behind(d), d)) + [r])
    done = [{} for _ in range(rings)]
    merges = [[0] * len(slots) for _ in range(rings)]
    for s in range(crosses + keeps):
        for r in range(rings):
            k = len(done[r])
            if k == keeps or place[1, k] > s or place[0, k] + 3 > s:
                continue
            d, i = orders[r][k // parts], k % parts
            before = r - 1 if d > r else r + 1
            if 0 <= before < rings and done[before].get((d, i), s) + 3 > s:
                continue
            done[r][d, i] = s
            merges[r][s] = k + 1
    complete = all(len(d) == keeps for d in done)
    return slots, orders, merges, complete


def pick(values, i):
    out = values[-1]
    for k in reversed(range(len(values) - 1)):
        if values[k] != values[k + 1] or not isinstance(out, (int, float)):
            out = jnp.where(i == k, values[k], out)
    return out


def pick_row(rows, r, i):
    out = None
    unique = []
    for row in rows:
        if row not in unique:
            unique.append(row)
    for row in unique:
        mine = pick(row, i)
        if out is None:
            out = mine
        else:
            here = functools.reduce(jnp.logical_or, [r == k for k in range(len(rows)) if rows[k] == row])
            out = jnp.where(here, mine, out)
    return out


def column(row):
    return jnp.transpose(jnp.broadcast_to(row, (LANES, LANES)))


def spread(square, total, share):
    return jnp.maximum(square - total * total * share, square * 1e-5 + 1e-30)


def encode(q):
    size = jnp.clip(jnp.abs(q), 1e-30, 1.04)
    size = jnp.exp2(size * lax.rsqrt(size) * SPAN - BASE)
    return jnp.where(q < 0, -size, size).astype(jnp.bfloat16)


def decode(code):
    y = code.astype(jnp.float32)
    size = jnp.log2(jnp.abs(y)) + BASE
    size = size * size
    return jnp.where(y < 0, -size, size)


def work(groups, plan, a_hbm, b_hbm, out, a, g, held, cross_out, cross_in, far_out, far_in,
           sa_own, sa_near, sa_pair, sa_in, sa_run, sa_stat, sb_half, sb_mine, sb_near, sb_run, sb_in,
           a_sem, b_sem, px_send, px_recv, nx_send, nx_recv, fw_send, fw_recv,
           c_send, cb_send, c_recv, f_send, fb_send, f_recv,
           ca_send, ca_recv, fa_send, fa_recv, ready, go):
    slots, orders, merges, _ = plan
    t = lax.axis_index("tok")
    u = lax.axis_index("unit")
    rows, units = b_hbm.shape
    tokens, own = a.shape
    band = units // groups
    parts = band // LANES
    rings = groups // 2
    crosses = rings * parts
    keeps = crosses - parts
    steps = len(slots)
    main = steps - parts
    bunch = steps // BUNCHES
    half = tokens // 2
    r = t // 2
    y = t % 2
    side = u // 2
    partner = u + 1 - 2 * (u % 2)
    across = (u + 2) % 4
    near = t + 1 - 2 * y
    shares = [1.0 / (2 * tokens * max(k, 1)) for k in range(rings + 1)]
    packed = [kind + 2 * (k // parts) + 2048 * (k % parts) for kind, k in slots]

    def slot(s):
        code = pick(packed, s)
        kind, p, i = code % 2, (code // 2) % 1024, code // 2048
        return kind, p, i

    def bound(p):
        return pick_row(orders, r, p)

    def columns(kind, p, i):
        owner = bound(p) * 2 + jnp.where(kind == 0, 1 - y, y)
        return pl.ds(pl.multiple_of(owner * band + i * LANES, LANES), LANES)

    def block(ref, who, cols):
        return ref.at[pl.ds(pl.multiple_of(who * rows, rows), rows), cols]

    def remote(src, dst, send, recv, tt, uu):
        return pltpu.make_async_remote_copy(
            src_ref=src, dst_ref=dst, send_sem=send, recv_sem=recv,
            device_id=(tt, uu), device_id_type=MESH)

    def to_partner(s, cols):
        return remote(b_hbm.at[:, cols], block(g, u, cols), px_send.at[0], px_recv.at[s // bunch], t, partner)

    def to_across(s, cols):
        return remote(block(g, u, cols), block(g, u, cols), nx_send.at[0], nx_recv.at[s % (2 * AHEAD)],
                      t, across)

    def forward(s, cols):
        return remote(block(g, across, cols), block(g, across, cols), fw_send.at[0],
                      fw_recv.at[2 * (s % 2)], t, partner)

    def piece(who, h, cols):
        size = rows // 2
        return g.at[pl.ds(pl.multiple_of(who * rows + h * size, size), size), cols]

    def last_across(i, h, cols):
        return remote(piece(u, h, cols), piece(u, h, cols),
                      nx_send.at[0], nx_recv.at[2 * AHEAD + 2 * i + h], t, across)

    def last_forward(s, h, cols):
        return remote(piece(across, h, cols), piece(across, h, cols), fw_send.at[0],
                      fw_recv.at[2 * (s % 2) + h], t, partner)

    def issue_across(s):
        cols = columns(*slot(s))

        @pl.when(s < main)
        def _():
            to_across(s, cols).start()

        @pl.when(jnp.logical_and(s >= main, s < steps))
        def _():
            for h in (0, 1):
                last_across(s - main, h, cols).start()

    def send_cross(k):
        return remote(cross_out.at[k], cross_in.at[k], c_send.at[0], c_recv.at[k], near, u)

    def send_cross_sums(k):
        return remote(sb_mine.at[k], sb_near.at[k], cb_send.at[0], c_recv.at[k], near, u)

    def both(sem):
        some = g.at[pl.ds(0, own + 16), pl.ds(0, LANES)]
        return pltpu.make_async_copy(some, some, sem)

    def send_far(k, j, tt):
        return remote(far_out.at[k], far_in.at[j], f_send.at[0], f_recv.at[j], tt, u)

    def send_far_sums(k, j, tt):
        return remote(sb_run.at[k], sb_in.at[j], fb_send.at[0], f_recv.at[j], tt, u)

    send_near_a = remote(sa_own, sa_near, ca_send.at[0], ca_recv.at[0], near, u)

    def send_run_a(way):
        tt = t + 2 if way == 0 else t - 2
        return remote(sa_run.at[way], sa_in.at[way], fa_send.at[way], fa_recv.at[way], tt, u)

    a_copy = pltpu.make_async_copy(a_hbm, a, a_sem)
    own_rows = pl.ds(pl.multiple_of(u * rows, rows), rows)

    def b_copy(s):
        cols = columns(*slot(s))
        return pltpu.make_async_copy(
            b_hbm.at[:, cols], g.at[own_rows, cols], b_sem.at[jnp.where(s == 0, 0, jnp.where(s < AHEAD, 1, 2))])

    def b_wait(which, count):
        cols = pl.ds(0, LANES * count)
        pltpu.make_async_copy(b_hbm.at[:, cols], g.at[own_rows, cols], b_sem.at[which]).wait()

    barrier = pltpu.get_barrier_semaphore()

    early_core = u % 2 == 0
    wide_core = u % 2 == 1
    peers = 1 + jnp.where(r > 0, 1, 0) + jnp.where(r < rings - 1, 1, 0)

    def tell(sem, tt, uu):
        pl.semaphore_signal(sem, inc=1, device_id=(tt, uu), device_id_type=MESH)

    def tell_peers(sem):
        tell(sem, near, u)

        @pl.when(r > 0)
        def _():
            tell(sem, t - 2, u)

        @pl.when(r < rings - 1)
        def _():
            tell(sem, t + 2, u)

    tell(barrier, t, across)
    tell(barrier, t, partner)

    @pl.when(wide_core)
    def _():
        tell_peers(barrier)

    @pl.loop(0, AHEAD)
    def _(s):
        b_copy(s).start()

    a_copy.start()
    pl.semaphore_wait(barrier, 2 + jnp.where(wide_core, peers, 0))

    @pl.when(wide_core)
    def _():
        tell_peers(ready)

    first = columns(*slot(jnp.int32(0)))
    remote(b_hbm.at[:, first], block(g, u, first), nx_send.at[0], nx_recv.at[0], t, across).start()
    b_wait(0, 1)
    b_wait(1, AHEAD - 1)

    @pl.loop(1, AHEAD)
    def _(s):
        issue_across(s)

    @pl.loop(0, steps)
    def _(s):
        to_partner(s, columns(*slot(s))).start()

        @pl.when(s >= AHEAD)
        def _():
            b_copy(s).start()

    b_wait(2, steps - AHEAD)
    a_copy.wait()
    chunk = 128

    def sum_rows(wide):
        wide = wide.astype(jnp.float32).reshape(wide.shape[0] // 8, 8, wide.shape[1])
        return jnp.sum(wide, axis=0), jnp.sum(wide * wide, axis=0)

    def body(i, carry):
        total, square = sum_rows(a[pl.ds(pl.multiple_of(i * chunk, chunk), chunk), :])
        return carry[0] + total, carry[1] + square

    zero = jnp.zeros((8, own), jnp.float32)
    total, square = lax.fori_loop(0, tokens // chunk, body, (zero, zero))
    sa_own[...] = jnp.zeros((8, own), jnp.float32)
    sa_own[0:1, :] = jnp.sum(total, axis=0, keepdims=True)
    sa_own[1:2, :] = jnp.sum(square, axis=0, keepdims=True)

    @pl.when(wide_core)
    def _():
        pl.semaphore_wait(ready, peers)
        tell(go, t, partner)

    @pl.when(early_core)
    def _():
        pl.semaphore_wait(go, 1)

    send_near_a.start()

    def tiles():
        return [slice(c * LANES, (c + 1) * LANES) for c in range(own // LANES)]

    def early(hold, cols):
        mine = pl.ds(pl.multiple_of(side * half, half), half)
        lhs = g[mine, cols]
        held[hold] = contract_tokens(lhs, a[mine, :])
        total, square = sum_rows(lhs)
        sb_half[0] = total
        sb_half[1] = square

    def part(hold, start, size, cols):
        some = pl.ds(pl.multiple_of(start, size), size)
        lhs = g[some, cols]
        held[hold] = held[hold] + contract_tokens(lhs, a[some, :])
        total, square = sum_rows(lhs)
        sb_half[0] = sb_half[0] + total
        sb_half[1] = sb_half[1] + square

    def finish_sums(k):
        sb_mine[k] = jnp.zeros((8, LANES), jnp.float32)
        sb_mine[k, 0:1, :] = jnp.sum(sb_half[0], axis=0, keepdims=True)
        sb_mine[k, 1:2, :] = jnp.sum(sb_half[1], axis=0, keepdims=True)

    def put(target, k, hold, sb, sa, share):
        tb, qb = sb[0:1, :], sb[1:2, :]
        tb_col = column(tb * share)
        scale_col = column(lax.rsqrt(spread(qb, tb, share)))
        for cols in tiles():
            ta = sa[0:1, cols]
            scale = lax.rsqrt(spread(sa[1:2, cols], ta, share))
            q = (held[hold, :, cols] - tb_col * ta) * (scale_col * scale)
            target[k, :, cols] = encode(q)

    def take(hold, source, k, sb, sa, share):
        tb, qb = sb[0:1, :], sb[1:2, :]
        tb_col = column(tb * share)
        norm_col = column(jnp.sqrt(spread(qb, tb, share)) * (1.0 / (SPAN * SPAN)))
        for cols in tiles():
            ta = sa[0:1, cols]
            norm = jnp.sqrt(spread(sa[1:2, cols], ta, share))
            held[hold, :, cols] = held[hold, :, cols] + (
                decode(source[k, :, cols]) * (norm_col * norm) + tb_col * ta)

    def take_near(k):
        both(c_recv.at[k]).wait()
        take(k, cross_in, k, sb_near.at[k], sa_near, 1.0 / tokens)

    def take_far(way, k, j):
        both(f_recv.at[j]).wait()
        count = jnp.where(way == 0, r, rings - 1 - r)
        take(k, far_in, j, sb_in.at[j], sa_in.at[way], pick(shares, count))

    def route(k):
        p, i = k // parts, k % parts
        d = bound(p)
        way = jnp.where(d > r, 0, 1)
        count = jnp.where(way == 0, r, rings - 1 - r)
        distance = jnp.where(way == 0, d - r, r - d)
        return way, count, (way * (rings - 1) + distance) * parts + i

    def collect(k):
        way, count, j = route(k)
        take_near(k)

        @pl.when(count > 0)
        def _():
            take_far(way, k, j)

    def pass_on(k):
        way, count, j = route(k)
        sb_run[k] = sb_mine[crosses + k] + sb_near[k]

        @pl.when(count > 0)
        def _():
            sb_run[k] = sb_run[k] + sb_in[j]

        put(far_out, k, k, sb_run.at[k], sa_run.at[way], pick(shares, count + 1))
        tt = t + 2 - 4 * way
        send_far(k, j - parts, tt).start()
        send_far_sums(k, j - parts, tt).start()

    def exchange_a(s):
        @pl.when(s == 1)
        def _():
            send_near_a.wait_recv()
            sa_pair[...] = sa_own[...] + sa_near[...]

        for way, ready in ((0, r + 1), (1, rings - r)):
            first = (r == 0) if way == 0 else (r == rings - 1)
            final = (r == rings - 1) if way == 0 else (r == 0)

            @pl.when(jnp.logical_and(s == ready, first))
            def _():
                sa_in[way] = jnp.zeros((8, own), jnp.float32)
                sa_run[way] = sa_pair[...]

            @pl.when(jnp.logical_and(s == ready, jnp.logical_not(first)))
            def _():
                send_run_a(way).wait_recv()
                sa_run[way] = sa_pair[...] + sa_in[way]

            @pl.when(jnp.logical_and(s == ready, jnp.logical_not(final)))
            def _():
                send_run_a(way).start()

    def partner_ready(s):
        @pl.when(s % bunch == 0)
        def _():
            to_partner(s, pl.ds(0, LANES * bunch)).wait_recv()

    @pl.loop(0, main)
    def _(s):
        kind, p, i = slot(s)
        cols = columns(kind, p, i)
        k = p * parts + i
        hold = jnp.where(kind == 0, crosses, k)
        partner_ready(s)
        early(hold, cols)
        to_across(s, cols).wait_recv()
        forward(s, cols).start()
        issue_across(s + AHEAD)
        exchange_a(s)
        pair = pick_row(merges, r, s)

        @pl.when(pair > 0)
        def _():
            collect(pair - 1)

        part(hold, across * rows, rows, cols)
        forward(s, cols).wait_recv()
        part(hold, (across + 1 - 2 * (across % 2)) * rows, rows, cols)
        finish_sums(kind * crosses + k)

        @pl.when(kind == 0)
        def _():
            put(cross_out, k, hold, sb_mine.at[k], sa_own, 1.0 / tokens)
            send_cross(k).start()
            send_cross_sums(k).start()

        @pl.when(pair > 0)
        def _():
            pass_on(pair - 1)

    whole_a = sa_pair[...] + sa_in[0] + sa_in[1]
    total_tokens = tokens * groups
    mean_a = whole_a[0:1, :] * (1.0 / total_tokens)
    var_a = whole_a[1:2, :] * (1.0 / total_tokens) - mean_a * mean_a
    sa_stat[0:1, :] = mean_a
    sa_stat[1:2, :] = 1.0 / jnp.sqrt(var_a + 1e-05)

    @pl.loop(0, parts)
    def _(i):
        s = main + i
        k = keeps + i
        cols = pl.ds(pl.multiple_of(t * band + i * LANES, LANES), LANES)
        partner_ready(s)
        early(k, cols)
        take_near(k)
        sb_half[2] = sb_near[k]
        for h in (0, 1):
            last_across(i, h, cols).wait_recv()
            last_forward(s, h, cols).start()
            part(k, across * rows + h * (rows // 2), rows // 2, cols)
        for way, some in ((0, r > 0), (1, r < rings - 1)):
            @pl.when(some)
            def _():
                j = way * (rings - 1) * parts + i
                take_far(way, k, j)
                sb_half[2] = sb_half[2] + sb_in[j]

        for h in (0, 1):
            last_forward(s, h, cols).wait_recv()
            part(k, (across + 1 - 2 * (across % 2)) * rows + h * (rows // 2), rows // 2, cols)
        finish_sums(crosses + k)
        whole_b = sb_half[2] + sb_mine[crosses + k]
        mean_b = whole_b[0:1, :] * (1.0 / total_tokens)
        var_b = whole_b[1:2, :] * (1.0 / total_tokens) - mean_b * mean_b
        mean_col = column(mean_b)
        inv_col = column(1.0 / jnp.sqrt(var_b + 1e-05))
        lanes = pl.ds(pl.multiple_of(i * LANES, LANES), LANES)
        for c in tiles():
            centered = held[k, :, c] * (1.0 / total_tokens) - mean_col * sa_stat[0:1, c]
            out[lanes, c] = centered * (inv_col * sa_stat[1:2, c])

    send_near_a.wait_send()

    @pl.when(r < rings - 1)
    def _():
        send_run_a(0).wait_send()

    @pl.when(r > 0)
    def _():
        send_run_a(1).wait_send()

    own_b = g.at[own_rows, :]
    remote(own_b, own_b, nx_send.at[0], nx_recv.at[0], t, across).wait_send()
    remote(b_hbm, own_b, px_send.at[0], px_recv.at[0], t, partner).wait_send()
    remote(own_b, own_b, fw_send.at[0], fw_recv.at[0], t, partner).wait_send()
    remote(cross_out, cross_in, c_send.at[0], c_recv.at[0], near, u).wait_send()
    remote(sb_near, sb_near, cb_send.at[0], c_recv.at[0], near, u).wait_send()
    remote(far_out, far_out, f_send.at[0], f_recv.at[0], near, u).wait_send()
    remote(sb_run, sb_run, fb_send.at[0], f_recv.at[0], near, u).wait_send()


def kernel(groups, plan, semaphores, *refs):
    pl.run_scoped(lambda *sems: work(groups, plan, *refs, *sems), *semaphores)


def fused(groups, plan, act_a, act_b):
    tokens, own = act_a.shape
    rows, units = act_b.shape
    band = units // groups
    parts = band // LANES
    rings = groups // 2
    crosses = rings * parts
    keeps = crosses - parts
    steps = 2 * crosses
    dma = lambda n: pltpu.SemaphoreType.DMA((n,))
    bf16 = lambda *shape: pltpu.VMEM(shape, jnp.bfloat16)
    f32 = lambda *shape: pltpu.VMEM(shape, jnp.float32)
    semaphores = [
        pltpu.SemaphoreType.DMA, dma(3),
        dma(1), dma(BUNCHES),
        dma(1), dma(2 * AHEAD + 2 * parts),
        dma(1), dma(4),
        dma(1), dma(1), dma(crosses),
        dma(1), dma(1), dma(2 * keeps),
        dma(1), dma(1),
        dma(2), dma(2),
        pltpu.SemaphoreType.REGULAR, pltpu.SemaphoreType.REGULAR,
    ]
    return pl.pallas_call(
        functools.partial(kernel, groups, plan, semaphores),
        out_shape=jax.ShapeDtypeStruct((band, own), jnp.float32),
        in_specs=[pl.BlockSpec(memory_space=pltpu.HBM)] * 2,
        out_specs=pl.BlockSpec(memory_space=pltpu.VMEM),
        scratch_shapes=[
            bf16(tokens, own),
            bf16(tokens, units),
            f32(crosses + 1, LANES, own),
            bf16(crosses, LANES, own),
            bf16(crosses, LANES, own),
            bf16(keeps, LANES, own),
            bf16(2 * keeps, LANES, own),
            f32(8, own), f32(8, own), f32(8, own),
            f32(2, 8, own), f32(2, 8, own), f32(8, own),
            f32(3, 8, LANES),
            f32(2 * crosses, 8, LANES), f32(crosses, 8, LANES),
            f32(keeps, 8, LANES), f32(2 * keeps, 8, LANES),
        ],
        compiler_params=pltpu.CompilerParams(
            collective_id=0, has_side_effects=True, vmem_limit_bytes=52000 * 1024
        ),
        name="gather_correlate",
    )(act_a, act_b)


def solution(mesh):
    groups, split = mesh.shape["tok"], mesh.shape["unit"]

    def per_device(act_a, act_b):
        band = act_b.shape[1] // groups
        whole = act_a.shape[0] % 256 == 0 and act_a.shape[1] % LANES == 0
        whole = whole and act_a.shape[1] + 16 <= act_a.shape[0]
        if split == 4 and groups % 2 == 0 and groups > 4 and band % LANES == 0 and whole:
            plan = schedule(groups // 2, band // LANES)
            if plan[-1] and len(plan[0]) % BUNCHES == 0:
                return fused(groups, plan, act_a, act_b)
        return plain(act_a, act_b)

    placed = (P("tok", "unit"), P(("tok", "unit"), None))
    return jax.shard_map(
        per_device, mesh=mesh, in_specs=placed, out_specs=P("tok", "unit"), check_vma=False
    )
```

```python
import functools

import jax
import jax.numpy as jnp
from jax import lax
from jax.experimental import pallas as pl
from jax.experimental.pallas import tpu as pltpu
from jax.sharding import PartitionSpec as P

MESH = pl.DeviceIdType.MESH
LANES = 128
SPAN = 244.0
BASE = 122.0
AHEAD = 4
BUNCHES = 4


def contract_tokens(left, right):
    return lax.dot_general(
        left, right, (((0,), (0,)), ((), ())), preferred_element_type=jnp.float32
    )


def plain(act_a, act_b):
    token_rows = act_a.shape[0]
    units = act_b.shape[1]
    groups = lax.axis_size("tok")
    band = units // groups
    total_tokens = token_rows * groups
    wide_a = act_a.astype(jnp.float32)
    first_total = jnp.sum(wide_a, axis=0)
    first_square = jnp.sum(wide_a * wide_a, axis=0)
    piece = lax.all_gather(act_b, "unit", axis=0, tiled=True)
    product = contract_tokens(piece, act_a)
    wide_piece = piece.astype(jnp.float32)
    second_total = jnp.sum(wide_piece, axis=0)
    second_square = jnp.sum(wide_piece * wide_piece, axis=0)
    shares = lax.psum_scatter(product, "tok", scatter_dimension=0, tiled=True)
    first_all, first_square_all, second_all, second_square_all = lax.psum(
        (first_total, first_square, second_total, second_square), "tok"
    )
    offset = lax.axis_index("tok") * band
    second_own = lax.dynamic_slice_in_dim(second_all, offset, band, 0)
    second_square_own = lax.dynamic_slice_in_dim(second_square_all, offset, band, 0)
    mean_a = first_all / total_tokens
    var_a = first_square_all / total_tokens - mean_a * mean_a
    mean_b = second_own / total_tokens
    var_b = second_square_own / total_tokens - mean_b * mean_b
    centered = shares / total_tokens - mean_b[:, None] * mean_a[None, :]
    return centered / (jnp.sqrt(var_b + 1e-05)[:, None] * jnp.sqrt(var_a + 1e-05)[None, :])


def schedule(rings, parts):
    crosses, keeps = rings * parts, (rings - 1) * parts
    events = sorted(
        [((k + 0.25) / crosses, 0, k) for k in range(crosses)]
        + [((k + 1) / keeps, 1, k) for k in range(keeps)]
    )
    slots = [(kind, k) for _, kind, k in events] + [(1, keeps + i) for i in range(parts)]
    place = {slot: s for s, slot in enumerate(slots)}
    orders = []
    for r in range(rings):
        behind = lambda d: r if d > r else rings - 1 - r
        others = [d for d in range(rings) if d != r]
        orders.append(sorted(others, key=lambda d: (-abs(d - r), -behind(d), d)) + [r])
    done = [{} for _ in range(rings)]
    merges = [[0] * len(slots) for _ in range(rings)]
    for s in range(crosses + keeps):
        for r in range(rings):
            k = len(done[r])
            if k == keeps or place[1, k] > s or place[0, k] + 3 > s:
                continue
            d, i = orders[r][k // parts], k % parts
            before = r - 1 if d > r else r + 1
            if 0 <= before < rings and done[before].get((d, i), s) + 3 > s:
                continue
            done[r][d, i] = s
            merges[r][s] = k + 1
    complete = all(len(d) == keeps for d in done)
    return slots, orders, merges, complete


def pick(values, i):
    out = values[-1]
    for k in reversed(range(len(values) - 1)):
        if values[k] != values[k + 1] or not isinstance(out, (int, float)):
            out = jnp.where(i == k, values[k], out)
    return out


def pick_row(rows, r, i):
    out = None
    unique = []
    for row in rows:
        if row not in unique:
            unique.append(row)
    for row in unique:
        mine = pick(row, i)
        if out is None:
            out = mine
        else:
            here = functools.reduce(jnp.logical_or, [r == k for k in range(len(rows)) if rows[k] == row])
            out = jnp.where(here, mine, out)
    return out


def column(row):
    return jnp.transpose(jnp.broadcast_to(row, (LANES, LANES)))


def spread(square, total, share):
    return jnp.maximum(square - total * total * share, square * 1e-5 + 1e-30)


def encode(q):
    size = jnp.clip(jnp.abs(q), 1e-30, 1.04)
    size = jnp.exp2(size * lax.rsqrt(size) * SPAN - BASE)
    return jnp.where(q < 0, -size, size).astype(jnp.bfloat16)


def decode(code):
    y = code.astype(jnp.float32)
    size = jnp.log2(jnp.abs(y)) + BASE
    size = size * size
    return jnp.where(y < 0, -size, size)


def work(groups, plan, a_hbm, b_hbm, out, a, g, held, cross_out, cross_in, far_out, far_in,
           sa_own, sa_near, sa_pair, sa_in, sa_run, sa_stat, sb_half, sb_mine, sb_near, sb_run, sb_in,
           a_sem, b_sem, px_send, px_recv, nx_send, nx_recv, fw_send, fw_recv,
           c_send, cb_send, c_recv, f_send, fb_send, f_recv,
           ca_send, ca_recv, fa_send, fa_recv, ready, go):
    slots, orders, merges, _ = plan
    t = lax.axis_index("tok")
    u = lax.axis_index("unit")
    rows, units = b_hbm.shape
    tokens, own = a.shape
    band = units // groups
    parts = band // LANES
    rings = groups // 2
    crosses = rings * parts
    keeps = crosses - parts
    steps = len(slots)
    main = steps - parts
    bunch = steps // BUNCHES
    half = tokens // 2
    r = t // 2
    y = t % 2
    side = u // 2
    partner = u + 1 - 2 * (u % 2)
    across = (u + 2) % 4
    near = t + 1 - 2 * y
    shares = [1.0 / (2 * tokens * max(k, 1)) for k in range(rings + 1)]
    packed = [kind + 2 * (k // parts) + 2048 * (k % parts) for kind, k in slots]

    def slot(s):
        code = pick(packed, s)
        kind, p, i = code % 2, (code // 2) % 1024, code // 2048
        return kind, p, i

    def bound(p):
        return pick_row(orders, r, p)

    def columns(kind, p, i):
        owner = bound(p) * 2 + jnp.where(kind == 0, 1 - y, y)
        return pl.ds(pl.multiple_of(owner * band + i * LANES, LANES), LANES)

    def block(ref, who, cols):
        return ref.at[pl.ds(pl.multiple_of(who * rows, rows), rows), cols]

    def remote(src, dst, send, recv, tt, uu):
        return pltpu.make_async_remote_copy(
            src_ref=src, dst_ref=dst, send_sem=send, recv_sem=recv,
            device_id=(tt, uu), device_id_type=MESH)

    def to_partner(s, cols):
        return remote(b_hbm.at[:, cols], block(g, u, cols), px_send.at[0], px_recv.at[s // bunch], t, partner)

    def to_across(s, cols):
        return remote(block(g, u, cols), block(g, u, cols), nx_send.at[0], nx_recv.at[s % (2 * AHEAD)],
                      t, across)

    def forward(s, cols):
        return remote(block(g, across, cols), block(g, across, cols), fw_send.at[0],
                      fw_recv.at[2 * (s % 2)], t, partner)

    def piece(who, h, cols):
        size = rows // 2
        return g.at[pl.ds(pl.multiple_of(who * rows + h * size, size), size), cols]

    def last_across(i, h, cols):
        return remote(piece(u, h, cols), piece(u, h, cols),
                      nx_send.at[0], nx_recv.at[2 * AHEAD + 2 * i + h], t, across)

    def last_forward(s, h, cols):
        return remote(piece(across, h, cols), piece(across, h, cols), fw_send.at[0],
                      fw_recv.at[2 * (s % 2) + h], t, partner)

    def issue_across(s):
        cols = columns(*slot(s))

        @pl.when(s < main)
        def _():
            to_across(s, cols).start()

        @pl.when(jnp.logical_and(s >= main, s < steps))
        def _():
            for h in (0, 1):
                last_across(s - main, h, cols).start()

    def send_cross(k):
        return remote(cross_out.at[k], cross_in.at[k], c_send.at[0], c_recv.at[k], near, u)

    def send_cross_sums(k):
        return remote(sb_mine.at[k], sb_near.at[k], cb_send.at[0], c_recv.at[k], near, u)

    def both(sem):
        some = g.at[pl.ds(0, own + 16), pl.ds(0, LANES)]
        return pltpu.make_async_copy(some, some, sem)

    def send_far(k, j, tt):
        return remote(far_out.at[k], far_in.at[j], f_send.at[0], f_recv.at[j], tt, u)

    def send_far_sums(k, j, tt):
        return remote(sb_run.at[k], sb_in.at[j], fb_send.at[0], f_recv.at[j], tt, u)

    send_near_a = remote(sa_own, sa_near, ca_send.at[0], ca_recv.at[0], near, u)

    def send_run_a(way):
        tt = t + 2 if way == 0 else t - 2
        return remote(sa_run.at[way], sa_in.at[way], fa_send.at[way], fa_recv.at[way], tt, u)

    a_copy = pltpu.make_async_copy(a_hbm, a, a_sem)
    own_rows = pl.ds(pl.multiple_of(u * rows, rows), rows)

    def b_copy(s):
        cols = columns(*slot(s))
        return pltpu.make_async_copy(
            b_hbm.at[:, cols], g.at[own_rows, cols], b_sem.at[jnp.where(s == 0, 0, jnp.where(s < AHEAD, 1, 2))])

    def b_wait(which, count):
        cols = pl.ds(0, LANES * count)
        pltpu.make_async_copy(b_hbm.at[:, cols], g.at[own_rows, cols], b_sem.at[which]).wait()

    barrier = pltpu.get_barrier_semaphore()

    early_core = u % 2 == 0
    wide_core = u % 2 == 1
    peers = 1 + jnp.where(r > 0, 1, 0) + jnp.where(r < rings - 1, 1, 0)

    def tell(sem, tt, uu):
        pl.semaphore_signal(sem, inc=1, device_id=(tt, uu), device_id_type=MESH)

    def tell_peers(sem):
        tell(sem, near, u)

        @pl.when(r > 0)
        def _():
            tell(sem, t - 2, u)

        @pl.when(r < rings - 1)
        def _():
            tell(sem, t + 2, u)

    tell(barrier, t, across)
    tell(barrier, t, partner)

    @pl.when(wide_core)
    def _():
        tell_peers(barrier)

    @pl.loop(0, AHEAD)
    def _(s):
        b_copy(s).start()

    a_copy.start()
    pl.semaphore_wait(barrier, 2 + jnp.where(wide_core, peers, 0))

    @pl.when(wide_core)
    def _():
        tell_peers(ready)

    first = columns(*slot(jnp.int32(0)))
    remote(b_hbm.at[:, first], block(g, u, first), nx_send.at[0], nx_recv.at[0], t, across).start()
    b_wait(0, 1)
    b_wait(1, AHEAD - 1)

    @pl.loop(1, AHEAD)
    def _(s):
        issue_across(s)

    @pl.loop(0, steps)
    def _(s):
        to_partner(s, columns(*slot(s))).start()

        @pl.when(s >= AHEAD)
        def _():
            b_copy(s).start()

    b_wait(2, steps - AHEAD)
    a_copy.wait()
    chunk = 128

    def sum_rows(wide):
        wide = wide.astype(jnp.float32).reshape(wide.shape[0] // 8, 8, wide.shape[1])
        return jnp.sum(wide, axis=0), jnp.sum(wide * wide, axis=0)

    def body(i, carry):
        total, square = sum_rows(a[pl.ds(pl.multiple_of(i * chunk, chunk), chunk), :])
        return carry[0] + total, carry[1] + square

    zero = jnp.zeros((8, own), jnp.float32)
    total, square = lax.fori_loop(0, tokens // chunk, body, (zero, zero))
    sa_own[...] = jnp.zeros((8, own), jnp.float32)
    sa_own[0:1, :] = jnp.sum(total, axis=0, keepdims=True)
    sa_own[1:2, :] = jnp.sum(square, axis=0, keepdims=True)

    @pl.when(wide_core)
    def _():
        pl.semaphore_wait(ready, peers)
        tell(go, t, partner)

    @pl.when(early_core)
    def _():
        pl.semaphore_wait(go, 1)

    send_near_a.start()

    def tiles():
        return [slice(c * LANES, (c + 1) * LANES) for c in range(own // LANES)]

    def early(hold, cols):
        mine = pl.ds(pl.multiple_of(side * half, half), half)
        lhs = g[mine, cols]
        held[hold] = contract_tokens(lhs, a[mine, :])
        total, square = sum_rows(lhs)
        sb_half[0] = total
        sb_half[1] = square

    def term(start, size, cols):
        some = pl.ds(pl.multiple_of(start, size), size)
        lhs = g[some, cols]
        total, square = sum_rows(lhs)
        sb_half[0] = sb_half[0] + total
        sb_half[1] = sb_half[1] + square
        return contract_tokens(lhs, a[some, :])

    def part(hold, start, size, cols):
        held[hold] = held[hold] + term(start, size, cols)

    def finish_sums(k):
        sb_mine[k] = jnp.zeros((8, LANES), jnp.float32)
        sb_mine[k, 0:1, :] = jnp.sum(sb_half[0], axis=0, keepdims=True)
        sb_mine[k, 1:2, :] = jnp.sum(sb_half[1], axis=0, keepdims=True)

    def put(target, k, hold, sb, sa, share):
        tb, qb = sb[0:1, :], sb[1:2, :]
        tb_col = column(tb * share)
        scale_col = column(lax.rsqrt(spread(qb, tb, share)))
        for cols in tiles():
            ta = sa[0:1, cols]
            scale = lax.rsqrt(spread(sa[1:2, cols], ta, share))
            q = (held[hold, :, cols] - tb_col * ta) * (scale_col * scale)
            target[k, :, cols] = encode(q)

    def take(hold, source, k, sb, sa, share):
        tb, qb = sb[0:1, :], sb[1:2, :]
        tb_col = column(tb * share)
        norm_col = column(jnp.sqrt(spread(qb, tb, share)) * (1.0 / (SPAN * SPAN)))
        for cols in tiles():
            ta = sa[0:1, cols]
            norm = jnp.sqrt(spread(sa[1:2, cols], ta, share))
            held[hold, :, cols] = held[hold, :, cols] + (
                decode(source[k, :, cols]) * (norm_col * norm) + tb_col * ta)

    def take_near(k):
        both(c_recv.at[k]).wait()
        take(k, cross_in, k, sb_near.at[k], sa_near, 1.0 / tokens)

    def take_far(way, k, j):
        both(f_recv.at[j]).wait()
        count = jnp.where(way == 0, r, rings - 1 - r)
        take(k, far_in, j, sb_in.at[j], sa_in.at[way], pick(shares, count))

    def route(k):
        p, i = k // parts, k % parts
        d = bound(p)
        way = jnp.where(d > r, 0, 1)
        count = jnp.where(way == 0, r, rings - 1 - r)
        distance = jnp.where(way == 0, d - r, r - d)
        return way, count, (way * (rings - 1) + distance) * parts + i

    def collect(k):
        way, count, j = route(k)
        take_near(k)

        @pl.when(count > 0)
        def _():
            take_far(way, k, j)

    def pass_on(k):
        way, count, j = route(k)
        sb_run[k] = sb_mine[crosses + k] + sb_near[k]

        @pl.when(count > 0)
        def _():
            sb_run[k] = sb_run[k] + sb_in[j]

        put(far_out, k, k, sb_run.at[k], sa_run.at[way], pick(shares, count + 1))
        tt = t + 2 - 4 * way
        send_far(k, j - parts, tt).start()
        send_far_sums(k, j - parts, tt).start()

    def exchange_a(s):
        @pl.when(s == 1)
        def _():
            send_near_a.wait_recv()
            sa_pair[...] = sa_own[...] + sa_near[...]

        for way, ready in ((0, r + 1), (1, rings - r)):
            first = (r == 0) if way == 0 else (r == rings - 1)
            final = (r == rings - 1) if way == 0 else (r == 0)

            @pl.when(jnp.logical_and(s == ready, first))
            def _():
                sa_in[way] = jnp.zeros((8, own), jnp.float32)
                sa_run[way] = sa_pair[...]

            @pl.when(jnp.logical_and(s == ready, jnp.logical_not(first)))
            def _():
                send_run_a(way).wait_recv()
                sa_run[way] = sa_pair[...] + sa_in[way]

            @pl.when(jnp.logical_and(s == ready, jnp.logical_not(final)))
            def _():
                send_run_a(way).start()

    def partner_ready(s):
        @pl.when(s % bunch == 0)
        def _():
            to_partner(s, pl.ds(0, LANES * bunch)).wait_recv()

    @pl.loop(0, main)
    def _(s):
        kind, p, i = slot(s)
        cols = columns(kind, p, i)
        k = p * parts + i
        hold = jnp.where(kind == 0, crosses, k)
        partner_ready(s)
        early(hold, cols)
        to_across(s, cols).wait_recv()
        forward(s, cols).start()
        issue_across(s + AHEAD)
        exchange_a(s)
        pair = pick_row(merges, r, s)

        @pl.when(pair > 0)
        def _():
            collect(pair - 1)

        part(hold, across * rows, rows, cols)
        forward(s, cols).wait_recv()
        part(hold, (across + 1 - 2 * (across % 2)) * rows, rows, cols)
        finish_sums(kind * crosses + k)

        @pl.when(kind == 0)
        def _():
            put(cross_out, k, hold, sb_mine.at[k], sa_own, 1.0 / tokens)
            send_cross(k).start()
            send_cross_sums(k).start()

        @pl.when(pair > 0)
        def _():
            pass_on(pair - 1)

    whole_a = sa_pair[...] + sa_in[0] + sa_in[1]
    total_tokens = tokens * groups
    mean_a = whole_a[0:1, :] * (1.0 / total_tokens)
    var_a = whole_a[1:2, :] * (1.0 / total_tokens) - mean_a * mean_a
    sa_stat[0:1, :] = mean_a
    sa_stat[1:2, :] = 1.0 / jnp.sqrt(var_a + 1e-05)

    @pl.loop(0, parts)
    def _(i):
        s = main + i
        k = keeps + i
        cols = pl.ds(pl.multiple_of(t * band + i * LANES, LANES), LANES)
        partner_ready(s)
        early(k, cols)
        take_near(k)
        sb_half[2] = sb_near[k]
        for h in (0, 1):
            last_across(i, h, cols).wait_recv()
            last_forward(s, h, cols).start()
            part(k, across * rows + h * (rows // 2), rows // 2, cols)
        for way, some in ((0, r > 0), (1, r < rings - 1)):
            @pl.when(some)
            def _():
                j = way * (rings - 1) * parts + i
                take_far(way, k, j)
                sb_half[2] = sb_half[2] + sb_in[j]

        theirs = (across + 1 - 2 * (across % 2)) * rows
        last_forward(s, 0, cols).wait_recv()
        part(k, theirs, rows // 2, cols)
        last_forward(s, 1, cols).wait_recv()
        rest = term(theirs + rows // 2, rows // 2, cols)
        finish_sums(crosses + k)
        whole_b = sb_half[2] + sb_mine[crosses + k]
        mean_b = whole_b[0:1, :] * (1.0 / total_tokens)
        var_b = whole_b[1:2, :] * (1.0 / total_tokens) - mean_b * mean_b
        mean_col = column(mean_b)
        inv_col = column(1.0 / jnp.sqrt(var_b + 1e-05))
        lanes = pl.ds(pl.multiple_of(i * LANES, LANES), LANES)
        for c in tiles():
            centered = (held[k, :, c] + rest[:, c]) * (1.0 / total_tokens) - mean_col * sa_stat[0:1, c]
            out[lanes, c] = centered * (inv_col * sa_stat[1:2, c])

    send_near_a.wait_send()

    @pl.when(r < rings - 1)
    def _():
        send_run_a(0).wait_send()

    @pl.when(r > 0)
    def _():
        send_run_a(1).wait_send()

    own_b = g.at[own_rows, :]
    remote(own_b, own_b, nx_send.at[0], nx_recv.at[0], t, across).wait_send()
    remote(b_hbm, own_b, px_send.at[0], px_recv.at[0], t, partner).wait_send()
    remote(own_b, own_b, fw_send.at[0], fw_recv.at[0], t, partner).wait_send()
    remote(cross_out, cross_in, c_send.at[0], c_recv.at[0], near, u).wait_send()
    remote(sb_near, sb_near, cb_send.at[0], c_recv.at[0], near, u).wait_send()
    remote(far_out, far_out, f_send.at[0], f_recv.at[0], near, u).wait_send()
    remote(sb_run, sb_run, fb_send.at[0], f_recv.at[0], near, u).wait_send()


def kernel(groups, plan, semaphores, *refs):
    pl.run_scoped(lambda *sems: work(groups, plan, *refs, *sems), *semaphores)


def fused(groups, plan, act_a, act_b):
    tokens, own = act_a.shape
    rows, units = act_b.shape
    band = units // groups
    parts = band // LANES
    rings = groups // 2
    crosses = rings * parts
    keeps = crosses - parts
    steps = 2 * crosses
    dma = lambda n: pltpu.SemaphoreType.DMA((n,))
    bf16 = lambda *shape: pltpu.VMEM(shape, jnp.bfloat16)
    f32 = lambda *shape: pltpu.VMEM(shape, jnp.float32)
    semaphores = [
        pltpu.SemaphoreType.DMA, dma(3),
        dma(1), dma(BUNCHES),
        dma(1), dma(2 * AHEAD + 2 * parts),
        dma(1), dma(4),
        dma(1), dma(1), dma(crosses),
        dma(1), dma(1), dma(2 * keeps),
        dma(1), dma(1),
        dma(2), dma(2),
        pltpu.SemaphoreType.REGULAR, pltpu.SemaphoreType.REGULAR,
    ]
    return pl.pallas_call(
        functools.partial(kernel, groups, plan, semaphores),
        out_shape=jax.ShapeDtypeStruct((band, own), jnp.float32),
        in_specs=[pl.BlockSpec(memory_space=pltpu.HBM)] * 2,
        out_specs=pl.BlockSpec(memory_space=pltpu.VMEM),
        scratch_shapes=[
            bf16(tokens, own),
            bf16(tokens, units),
            f32(crosses + 1, LANES, own),
            bf16(crosses, LANES, own),
            bf16(crosses, LANES, own),
            bf16(keeps, LANES, own),
            bf16(2 * keeps, LANES, own),
            f32(8, own), f32(8, own), f32(8, own),
            f32(2, 8, own), f32(2, 8, own), f32(8, own),
            f32(3, 8, LANES),
            f32(2 * crosses, 8, LANES), f32(crosses, 8, LANES),
            f32(keeps, 8, LANES), f32(2 * keeps, 8, LANES),
        ],
        compiler_params=pltpu.CompilerParams(
            collective_id=0, has_side_effects=True, vmem_limit_bytes=52000 * 1024
        ),
        name="gather_correlate",
    )(act_a, act_b)


def solution(mesh):
    groups, split = mesh.shape["tok"], mesh.shape["unit"]

    def per_device(act_a, act_b):
        band = act_b.shape[1] // groups
        whole = act_a.shape[0] % 256 == 0 and act_a.shape[1] % LANES == 0
        whole = whole and act_a.shape[1] + 16 <= act_a.shape[0]
        if split == 4 and groups % 2 == 0 and groups > 4 and band % LANES == 0 and whole:
            plan = schedule(groups // 2, band // LANES)
            if plan[-1] and len(plan[0]) % BUNCHES == 0:
                return fused(groups, plan, act_a, act_b)
        return plain(act_a, act_b)

    placed = (P("tok", "unit"), P(("tok", "unit"), None))
    return jax.shard_map(
        per_device, mesh=mesh, in_specs=placed, out_specs=P("tok", "unit"), check_vma=False
    )
```
